256 devices in a mesh: ha: 8 (over z_lo, y), wa: 32 (over x, z_hi, core).
Axes of the slice: x: 4, y: 4, z: 8 (z_hi: 4, z_lo: 2; z = z_hi * 2 + z_lo), core: 2. Of those that a mesh axis runs over, the one named last changes fastest.
Arguments:
- block_input: bfloat16 [3, 184, 320, 128], P(None, 'ha', 'wa'), may hold values from -6 to 6
- cotangent: bfloat16 [3, 184, 320, 128], P(None, 'ha', 'wa'), may hold values from -6 to 6
- kernel_one: bfloat16 [3, 3, 3, 128, 128], replicated, may hold values from -0.109375 to 0.109375
- bias_one: float32 [128], replicated, may hold values from -3 to 3
- kernel_two: bfloat16 [3, 3, 3, 128, 128], replicated, may hold values from -0.109375 to 0.109375
- scale_one: float32 [128], replicated, may hold values from 0.5 to 2
- shift_one: float32 [128], replicated, may hold values from -1 to 1
- scale_two: float32 [128], replicated, may hold values from 0.5 to 2
- shift_two: float32 [128], replicated, may hold values from -1 to 1
Outputs:
- grad_input: bfloat16 [3, 184, 320, 128], P(None, 'ha', 'wa')
- grad_kernel_one: float32 [3, 3, 3, 128, 128], replicated
- grad_bias_one: float32 [128], replicated
- grad_kernel_two: float32 [3, 3, 3, 128, 128], replicated
- grad_bias_two: float32 [128], replicated
The draws below stay inside these ranges and needn't reach their ends.
All inputs are finite; a program needn't handle non-finite values.
Results may differ from the reference program's by a relative error of at most 0.0054.
Values may be sent and summed in bfloat16 or wider, within the bound.
No kernel may reach another device: no remote copies, remote signals or barrier semaphores. Data moves between devices by JAX's collectives and lax.ppermute only.
A program may use at most 64 MiB of HBM per device.

```python
import math
import jax
import jax.numpy as jnp
from jax import lax

CHANNELS = 128
FRAMES = 3
HEIGHT = 184
WIDTH = 320
CELLS = 176640


def level_of(stream_key, shape, split, least, largest):
    gain = 1.0
    for dim, parts in split:
        steps = jax.random.uniform(jax.random.fold_in(jax.random.fold_in(stream_key, 6), dim), (parts,), jnp.float32, least / len(split), largest / len(split))
        gain = gain * jnp.repeat(jnp.exp(steps), shape[dim] // parts).reshape((-1,) + (1,) * (len(shape) - 1 - dim))
    return gain


def noise(rng, dims, spread, limit, pieces=(), kind=jnp.bfloat16):
    entries = jax.random.normal(rng, dims, jnp.float32) * spread
    if len(pieces) > 0:
        entries = level_of(rng, dims, pieces, -0.22, 0.18) * entries
    return jnp.clip(entries, min=-limit, max=limit).astype(kind)


def setup_inputs(seed: int = 0) -> dict:
    key_list = jax.random.split(jax.random.key(seed), 10)
    return {
        "block_input": noise(key_list[0], (FRAMES, HEIGHT, WIDTH, CHANNELS), 1.0, 6.0, ((1, 8), (2, 32))),
        "cotangent": noise(key_list[1], (FRAMES, HEIGHT, WIDTH, CHANNELS), 1.0, 6.0, ((1, 8), (2, 32))),
        "kernel_one": noise(key_list[2], (3, 3, 3, CHANNELS, CHANNELS), (27 * CHANNELS) ** -0.5, 0.109375),
        "bias_one": noise(key_list[3], (CHANNELS,), 0.5, 3.0, (), jnp.float32),
        "kernel_two": noise(key_list[4], (3, 3, 3, CHANNELS, CHANNELS), (27 * CHANNELS) ** -0.5, 0.109375),
        "scale_one": jnp.clip(jnp.exp(jax.random.uniform(key_list[5], (CHANNELS,), jnp.float32, math.log(0.5), math.log(2.0))), 0.5, 2.0),
        "shift_one": jnp.clip(jax.random.uniform(key_list[6], (CHANNELS,), jnp.float32, -1.0, 1.0), -1.0, 1.0),
        "scale_two": jnp.clip(jnp.exp(jax.random.uniform(key_list[7], (CHANNELS,), jnp.float32, math.log(0.5), math.log(2.0))), 0.5, 2.0),
        "shift_two": jnp.clip(jax.random.uniform(key_list[8], (CHANNELS,), jnp.float32, -1.0, 1.0), -1.0, 1.0),
    }


def convolve(field, kernel):
    out = lax.conv_general_dilated(field[None], kernel, (1, 1, 1), ((2, 0), (1, 1), (1, 1)), dimension_numbers=('NDHWC', 'DHWIO', 'NDHWC'), precision=lax.Precision.HIGHEST)
    return out[0]

def slope(value):
    sigma = jax.nn.sigmoid(value)
    return sigma * (1.0 + value * (1.0 - sigma))

def reference(block_input, cotangent, kernel_one, bias_one, kernel_two, scale_one, shift_one, scale_two, shift_two):
    factor = 1.0 / math.sqrt(CELLS)
    first_pre = block_input.astype(jnp.float32) * scale_one + shift_one
    first_act = jax.nn.silu(first_pre).astype(jnp.bfloat16)
    first_f = first_act.astype(jnp.float32)
    kernel_a = kernel_one.astype(jnp.float32)
    kernel_b = kernel_two.astype(jnp.float32)
    hidden = convolve(first_f, kernel_a) + bias_one
    second_pre = hidden * scale_two + shift_two
    second_act = jax.nn.silu(second_pre).astype(jnp.bfloat16)
    upstream = cotangent.astype(jnp.float32)
    unused, pull_two = jax.vjp(convolve, second_act.astype(jnp.float32), kernel_b)
    back_two, grad_two = pull_two(upstream)
    inner = (back_two * slope(second_pre) * scale_two).astype(jnp.bfloat16)
    unused, pull_one = jax.vjp(convolve, first_f, kernel_a)
    back_one, grad_one = pull_one(inner.astype(jnp.float32))
    grad_input = (upstream + back_one * slope(first_pre) * scale_one).astype(jnp.bfloat16)
    bias_a = lax.optimization_barrier(jnp.sum(inner.astype(jnp.float32), axis=(0, 1, 2)))
    bias_b = lax.optimization_barrier(jnp.sum(upstream, axis=(0, 1, 2)))
    return (grad_input, grad_one * factor, bias_a * factor, grad_two * factor, bias_b * factor)
```

```python
import math

import jax
import jax.numpy as jnp
from jax import lax
from jax.sharding import PartitionSpec as P

CELLS = 176640
AXES = ("ha", "wa")
f32 = jnp.float32
bf16 = jnp.bfloat16


def coords(d):
    return {"zl": d // 128, "y": (d // 32) % 4, "x": (d // 8) % 4, "zh": (d // 2) % 4, "c": d % 2}


def device_of(p):
    return (((p["zl"] * 4 + p["y"]) * 4 + p["x"]) * 4 + p["zh"]) * 2 + p["c"]


def shift_pairs(axis, size, k):
    pairs = []
    for d in range(256):
        p = coords(d)
        p[axis] = (p[axis] + k) % size
        pairs.append((d, device_of(p)))
    return pairs


def shifted(v, axis, size, k):
    return lax.ppermute(v, AXES, shift_pairs(axis, size, k))


def scatter(v, axis, size, here, dtype):
    own = lax.dynamic_index_in_dim(v, here, 0, keepdims=False)
    got = [
        shifted(lax.dynamic_index_in_dim(v, (here + k) % size, 0, keepdims=False).astype(dtype), axis, size, k)
        for k in range(1, size)
    ]
    for g in got:
        own = own + g.astype(f32)
    return own


def gather(v, axis, size, here):
    out = jnp.zeros((size,) + v.shape, v.dtype)
    out = lax.dynamic_update_index_in_dim(out, v, here, 0)
    got = [shifted(v, axis, size, k) for k in range(1, size)]
    for k, g in enumerate(got, 1):
        out = lax.dynamic_update_index_in_dim(out, g, (here - k) % size, 0)
    return out


def total(v):
    ha, wa = lax.axis_index("ha"), lax.axis_index("wa")
    y, x, c = ha % 4, wa // 8, wa % 2
    v = scatter(v.reshape(2, 28, 128, 128), "c", 2, c, bf16)
    v = scatter(v.reshape(4, 7, 128, 128), "x", 4, x, bf16)
    v = scatter(v.reshape(4, 224, 128), "y", 4, y, f32)
    v = v + shifted(v, "zl", 2, 1)
    v = v.astype(bf16)
    a, b, d = (shifted(v, "zh", 4, k) for k in (2, 1, 3))
    v = ((v.astype(f32) + a.astype(f32)) + (b.astype(f32) + d.astype(f32))).astype(bf16)
    v = gather(v, "y", 4, y)
    v = gather(v, "x", 4, x)
    v = gather(v, "c", 2, c)
    return v.reshape(56, 128, 128)


def widen(v, axis, size, dim):
    n = v.shape[dim]
    up = [(i, i + 1) for i in range(size - 1)]
    down = [(i + 1, i) for i in range(size - 1)]
    before = lax.ppermute(lax.slice_in_dim(v, n - 2, n, axis=dim), axis, up)
    after = lax.ppermute(lax.slice_in_dim(v, 0, 2, axis=dim), axis, down)
    return jnp.concatenate([before, v, after], axis=dim)


def conv(field, kernel, time):
    out = lax.conv_general_dilated(
        field[None], kernel, (1, 1, 1), (time, (0, 0), (0, 0)),
        dimension_numbers=("NDHWC", "DHWIO", "NDHWC"), preferred_element_type=f32,
    )
    return out[0]


def adjoint(field, kernel):
    return conv(field, jnp.swapaxes(kernel[::-1, ::-1, ::-1], 3, 4), (0, 2))


def kernel_grad(field, cot):
    return lax.conv_general_dilated(
        field[None], cot[None], (1, 1, 1), ((2, 0), (0, 0), (0, 0)),
        dimension_numbers=("CDHWN", "IDHWO", "DHWNC"), preferred_element_type=f32,
    )


def slope(value, sigma):
    return sigma * (1.0 + value * (1.0 - sigma))


def body(block_input, cotangent, kernel_one, bias_one, kernel_two, scale_one, shift_one, scale_two, shift_two):
    both = jnp.stack([block_input, cotangent])
    both = widen(both, "ha", 8, 2)
    both = widen(both, "wa", 32, 3)
    wide_in, wide_cot = both[0], both[1]
    rows = lax.axis_index("ha") * 23 - 2 + jnp.arange(27)
    cols = lax.axis_index("wa") * 10 - 2 + jnp.arange(14)
    inside = ((rows >= 0) & (rows < 184))[:, None] & ((cols >= 0) & (cols < 320))[None, :]
    inside = inside[None, :, :, None]

    z1 = wide_in.astype(f32) * scale_one + shift_one
    s1 = jax.nn.sigmoid(z1)
    a1 = jnp.where(inside, z1 * s1, 0.0).astype(bf16)
    z2 = (conv(a1, kernel_one, (2, 0)) + bias_one) * scale_two + shift_two
    inside2 = inside[:, 1:-1, 1:-1]
    s2 = jax.nn.sigmoid(z2)
    a2 = jnp.where(inside2, z2 * s2, 0.0).astype(bf16)
    da2 = adjoint(wide_cot, kernel_two)
    dc1 = jnp.where(inside2, da2 * slope(z2, s2) * scale_two, 0.0).astype(bf16)
    da1 = adjoint(dc1, kernel_one)
    z1o, s1o = z1[:, 2:-2, 2:-2], s1[:, 2:-2, 2:-2]
    grad_input = (cotangent.astype(f32) + da1 * slope(z1o, s1o) * scale_one).astype(bf16)
    own = dc1[:, 1:-1, 1:-1]
    grad_two = kernel_grad(a2, cotangent)
    grad_one = kernel_grad(a1[:, 1:-1, 1:-1], own)
    biases = jnp.stack([jnp.sum(own.astype(f32), (0, 1, 2)), jnp.sum(cotangent.astype(f32), (0, 1, 2))])
    partial = jnp.concatenate(
        [grad_one.reshape(27, 128, 128), grad_two.reshape(27, 128, 128),
         jnp.pad(biases, ((0, 254), (0, 0))).reshape(2, 128, 128)]
    )
    result = total(partial).astype(f32) * (1.0 / math.sqrt(CELLS))
    return (
        grad_input,
        result[:27].reshape(3, 3, 3, 128, 128),
        result[54, 0],
        result[27:54].reshape(3, 3, 3, 128, 128),
        result[54, 1],
    )


def solution(mesh):
    split = P(None, "ha", "wa", None)
    return jax.shard_map(
        body,
        mesh=mesh,
        in_specs=(split, split) + (P(),) * 7,
        out_specs=(split,) + (P(),) * 4,
        check_vma=False,
    )
```

```python
import math

import jax
import jax.numpy as jnp
from jax import lax
from jax.experimental import pallas as pl
from jax.experimental.pallas import tpu as pltpu
from jax.sharding import PartitionSpec as P

CELLS = 176640
AXES = ("ha", "wa")
f32 = jnp.float32
bf16 = jnp.bfloat16


def coords(d):
    return {"zl": d // 128, "y": (d // 32) % 4, "x": (d // 8) % 4, "zh": (d // 2) % 4, "c": d % 2}


def device_of(p):
    return (((p["zl"] * 4 + p["y"]) * 4 + p["x"]) * 4 + p["zh"]) * 2 + p["c"]


def shift_pairs(axis, size, k):
    pairs = []
    for d in range(256):
        p = coords(d)
        a = axis if isinstance(axis, str) else axis[p["c"]]
        p[a] = (p[a] + k) % size
        pairs.append((d, device_of(p)))
    return pairs


def shifted(v, axis, size, k):
    return lax.ppermute(v, AXES, shift_pairs(axis, size, k))


def scatter(v, axis, size, here, dtype):
    own = lax.dynamic_index_in_dim(v, here, 0, keepdims=False)
    got = [
        shifted(lax.dynamic_index_in_dim(v, (here + k) % size, 0, keepdims=False).astype(dtype), axis, size, k)
        for k in range(1, size)
    ]
    for g in got:
        own = own + g.astype(f32)
    return own


def gather(v, axis, size, here):
    out = jnp.zeros((size,) + v.shape, v.dtype)
    out = lax.dynamic_update_index_in_dim(out, v, here, 0)
    got = [shifted(v, axis, size, k) for k in range(1, size)]
    for k, g in enumerate(got, 1):
        out = lax.dynamic_update_index_in_dim(out, g, (here - k) % size, 0)
    return out


def total(own, send):
    ha, wa = lax.axis_index("ha"), lax.axis_index("wa")
    y, x, c = ha % 4, wa // 8, wa % 2
    first, second = jnp.where(c == 0, x, y), jnp.where(c == 0, y, x)
    v = own + shifted(send, "c", 2, 1).astype(f32)
    v = scatter(v.reshape(4, 7, 128, 128), ("x", "y"), 4, first, bf16)
    v = scatter(v.reshape(4, 224, 128), ("y", "x"), 4, second, f32)
    v = v + shifted(v, "zl", 2, 1)
    v = v.astype(bf16)
    a, b, d = (shifted(v, "zh", 4, k) for k in (2, 1, 3))
    v = ((v.astype(f32) + a.astype(f32)) + (b.astype(f32) + d.astype(f32))).astype(bf16)
    v = gather(v, ("y", "x"), 4, second)
    v = gather(v, ("x", "y"), 4, first)
    v = gather(v, "c", 2, c)
    return v.reshape(56, 128, 128)


def exchange(low, high, axis, size):
    up = [(i, i + 1) for i in range(size - 1)]
    down = [(i + 1, i) for i in range(size - 1)]
    return lax.ppermute(high, axis, up), lax.ppermute(low, axis, down)


def local_kernel(
    pos, xin, cot, sides, ends, k1, k2, bias1, scale1, shift1, scale2, shift2,
    gin, own_out, send_out,
    line, x_all, a3, g3, g3own, d3, d3own, a1t, a2t, acc, acc2, ds1,
):
    row0, col0, core = pos[0], pos[1], pos[2]
    line[...] = jnp.zeros_like(line)
    x_all[...] = jnp.zeros_like(x_all)
    g3own[...] = jnp.zeros_like(g3own)
    d3own[...] = jnp.zeros_like(d3own)

    def masks(first, n):
        q = lax.broadcasted_iota(jnp.int32, (n, 128), 0)
        col, row = (q >> 5) + first, q & 31
        own = (row >= 2) & (row < 25) & (col >= 2) & (col < 12)
        r, c = row + row0, col + col0
        inside = (r >= 0) & (r < 184) & (c >= 0) & (c < 320)
        return own, inside

    def spread(dst, t, first, n, order):
        for k, o in enumerate(order):
            dst[t, first:first + n, k * 128:(k + 1) * 128] = line[o:o + n, :].astype(bf16)

    def slope(z, s):
        return s * (1.0 + z * (1.0 - s))

    def place(dst, base, which, main, t):
        for w in range(14):
            at = base + w * 32
            if 2 <= w < 12:
                dst[at + 2:at + 25, :] = main[t, w - 2].astype(f32)
            else:
                dst[at + 2:at + 25, :] = sides[w // 12, which, t, w % 12].astype(f32)
            dst[at:at + 2, :] = ends[0, which, t, w].astype(f32)
            dst[at + 25:at + 27, :] = ends[1, which, t, w].astype(f32)

    def enter(t, bias):
        own, inside = masks(0, 448)
        line[8:456, :] = jnp.zeros((448, 128), f32)
        place(line, 8, 1, cot, t)
        place(x_all, 0, 0, xin, t)
        spread(g3, t, 0, 448, (9, 8, 7))
        go = jnp.where(own, line[8:456, :], 0.0)
        line[8:456, :] = go
        spread(g3own, t, 0, 448, (9, 8, 7))
        z = x_all[...] * scale1[...] + shift1[...]
        s = jax.nn.sigmoid(z)
        line[8:456, :] = jnp.where(inside, z * s, 0.0)
        spread(a3, t, 0, 448, (7, 8, 9))
        a1t[t] = jnp.transpose(line[40:552, :]).astype(bf16)
        ds1[t] = (slope(z, s) * scale1[...])[64:384, :]
        return bias + jnp.sum(go.reshape(56, 8, 128), axis=0)

    bias_two = lax.fori_loop(0, 3, enter, jnp.zeros((8, 128), f32))

    def nt(a, k, kt, kw):
        w = jnp.concatenate([k[kt, kh, kw] for kh in range(3)], axis=1)
        return lax.dot_general(a, w, (((1,), (1,)), ((), ())), preferred_element_type=f32)

    def rows(i, n):
        return pl.ds(pl.multiple_of(i * 32, 32), n)

    for t in range(3):
        acc[t] = jnp.zeros((384, 128), f32)
        acc2[t] = jnp.zeros((384, 128), f32)

    def first_convs(kw, carry):
        for t in range(3):
            for kt in range(2 - t, 3):
                w = jnp.concatenate([k1[kt, kh, kw] for kh in range(3)], axis=0)
                acc[t] += jnp.dot(a3[t + kt - 2, rows(kw, 384), :], w, preferred_element_type=f32)
        for t in range(3):
            for kt in range(t, 3):
                acc2[t] += nt(g3[t - kt + 2, rows(2 - kw, 384), :], k2, kt, kw)
        return carry

    lax.fori_loop(0, 3, first_convs, 0)
    line[392:400, :] = jnp.zeros((8, 128), f32)

    def middle(t, bias):
        own, inside = masks(1, 384)
        z = (acc[t] + bias1[...]) * scale2[...] + shift2[...]
        s = jax.nn.sigmoid(z)
        line[8:392, :] = jnp.where(inside, z * s, 0.0)
        a2t[t] = jnp.transpose(line[8:520, :]).astype(bf16)
        d = jnp.where(inside, acc2[t] * slope(z, s) * scale2[...], 0.0)
        line[8:392, :] = d
        spread(d3, t, 0, 384, (9, 8, 7))
        do = jnp.where(own, d.astype(bf16).astype(f32), 0.0)
        line[8:392, :] = do
        spread(d3own, t, 32, 384, (9, 8, 7))
        return bias + jnp.sum(do.reshape(48, 8, 128), axis=0)

    bias_one = lax.fori_loop(0, 3, middle, jnp.zeros((8, 128), f32))

    for t in range(3):
        acc[t, 0:320, :] = jnp.zeros((320, 128), f32)

    def put(b, value):
        half = (b >= 28).astype(jnp.int32)
        at = b - half * 28

        @pl.when(half == core)
        def _():
            own_out[at] = value

        @pl.when(half != core)
        def _():
            send_out[at] = value.astype(bf16)

    def second_convs(kw, carry):
        for t in range(3):
            for kt in range(t, 3):
                acc[t, 0:320, :] += nt(d3[t - kt + 2, rows(2 - kw, 320), :], k1, kt, kw)
        for base, field, cotan in ((0, a1t, d3own), (27, a2t, g3own)):
            for kt in range(3):
                part = None
                for t in range(2 - kt, 3):
                    term = jnp.dot(field[t + kt - 2], cotan[t, rows(2 - kw, 512), :], preferred_element_type=f32)
                    part = term if part is None else part + term
                for kh in range(3):
                    put(base + kt * 9 + kh * 3 + kw, part[:, kh * 128:(kh + 1) * 128])
        return carry

    lax.fori_loop(0, 3, second_convs, 0)

    for t in range(3):
        value = acc[t, 0:320, :] * ds1[t]
        for w in range(10):
            gin[t, w] = (cot[t, w].astype(f32) + value[w * 32 + 2:w * 32 + 25, :]).astype(bf16)
    extra = lax.broadcasted_iota(jnp.int32, (128, 128), 0)
    b1 = jnp.broadcast_to(jnp.sum(bias_one, axis=0, keepdims=True), (128, 128))
    b2 = jnp.broadcast_to(jnp.sum(bias_two, axis=0, keepdims=True), (128, 128))
    put(jnp.int32(54), jnp.where(extra < 8, b1, jnp.where(extra < 16, b2, 0.0)))
    put(jnp.int32(55), jnp.zeros((128, 128), f32))


def local(pos, xin, cot, sides, ends, k1, k2, *vectors):
    vmem = pl.BlockSpec(memory_space=pltpu.VMEM)
    return pl.pallas_call(
        local_kernel,
        out_shape=(
            jax.ShapeDtypeStruct((3, 10, 23, 128), bf16),
            jax.ShapeDtypeStruct((28, 128, 128), f32),
            jax.ShapeDtypeStruct((28, 128, 128), bf16),
        ),
        in_specs=[pl.BlockSpec(memory_space=pltpu.SMEM)] + [vmem] * 11,
        out_specs=(vmem, vmem, vmem),
        scratch_shapes=[
            pltpu.VMEM((568, 128), f32),
            pltpu.VMEM((448, 128), f32),
            pltpu.VMEM((3, 448, 384), bf16),
            pltpu.VMEM((3, 448, 384), bf16),
            pltpu.VMEM((3, 576, 384), bf16),
            pltpu.VMEM((3, 384, 384), bf16),
            pltpu.VMEM((3, 576, 384), bf16),
            pltpu.VMEM((3, 128, 512), bf16),
            pltpu.VMEM((3, 128, 512), bf16),
            pltpu.VMEM((3, 384, 128), f32),
            pltpu.VMEM((3, 384, 128), f32),
            pltpu.VMEM((3, 320, 128), f32),
        ],
        compiler_params=pltpu.CompilerParams(vmem_limit_bytes=40 * 1024 * 1024),
        cost_estimate=pl.CostEstimate(flops=5 * 10**9, bytes_accessed=8 * 10**6, transcendentals=10**6),
    )(pos, xin, cot, sides, ends, k1, k2, *(v.reshape(1, 128) for v in vectors))

def body(block_input, cotangent, kernel_one, bias_one, kernel_two, scale_one, shift_one, scale_two, shift_two):
    xin, cot = jnp.swapaxes(block_input, 1, 2), jnp.swapaxes(cotangent, 1, 2)
    low = jnp.stack([xin[:, :2], cot[:, :2]])
    high = jnp.stack([xin[:, 8:], cot[:, 8:]])
    left, right = exchange(low, high, "wa", 32)

    def edge(s):
        main = jnp.stack([xin[:, :, s], cot[:, :, s]])
        return jnp.concatenate([left[:, :, :, s], main, right[:, :, :, s]], axis=2)

    above, below = exchange(edge(slice(0, 2)), edge(slice(21, 23)), "ha", 8)
    wa = lax.axis_index("wa")
    pos = jnp.stack([lax.axis_index("ha") * 23 - 2, wa * 10 - 2, wa % 2]).astype(jnp.int32)
    gin, own, send = local(
        pos, xin, cot, jnp.stack([left, right]), jnp.stack([above, below]), kernel_one, kernel_two,
        bias_one, scale_one, shift_one, scale_two, shift_two,
    )
    result = total(own, send).astype(f32) * (1.0 / math.sqrt(CELLS))
    return (
        jnp.swapaxes(gin, 1, 2),
        result[:27].reshape(3, 3, 3, 128, 128),
        result[54, 0],
        result[27:54].reshape(3, 3, 3, 128, 128),
        result[54, 8],
    )


def solution(mesh):
    split = P(None, "ha", "wa", None)
    return jax.shard_map(
        body,
        mesh=mesh,
        in_specs=(split, split) + (P(),) * 7,
        out_specs=(split,) + (P(),) * 4,
        check_vma=False,
    )
```

```python
import math

import jax
import jax.numpy as jnp
from jax import lax
from jax.experimental import pallas as pl
from jax.experimental.pallas import tpu as pltpu
from jax.sharding import PartitionSpec as P

CELLS = 176640
AXES = ("ha", "wa")
f32 = jnp.float32
bf16 = jnp.bfloat16


def coords(d):
    return {"zl": d // 128, "y": (d // 32) % 4, "x": (d // 8) % 4, "zh": (d // 2) % 4, "c": d % 2}


def device_of(p):
    return (((p["zl"] * 4 + p["y"]) * 4 + p["x"]) * 4 + p["zh"]) * 2 + p["c"]


def shift_pairs(axis, size, k):
    pairs = []
    for d in range(256):
        p = coords(d)
        a = axis if isinstance(axis, str) else axis[p["c"]]
        p[a] = (p[a] + k) % size
        pairs.append((d, device_of(p)))
    return pairs


def shifted(v, axis, size, k):
    return lax.ppermute(v, AXES, shift_pairs(axis, size, k))


ORDER = (2, 1, 3)


def scatter(own, send, axis):
    got = {k: shifted(send[k], axis, 4, k) for k in ORDER}
    return own + got[1].astype(f32) + got[2].astype(f32) + got[3].astype(f32)


def gather(v, axis, here):
    got = {k: shifted(v, axis, 4, k) for k in ORDER}
    out = lax.dynamic_update_index_in_dim(jnp.zeros((4,) + v.shape, v.dtype), v, here, 0)
    for k in (1, 3, 2):
        out = lax.dynamic_update_index_in_dim(out, got[k], (here - k) % 4, 0)
    return out


def total(pos, own, send):
    first, second = pos[3], pos[4]
    kept, *sends = combine(pos, own, shifted(send, "c", 2, 1))
    v = scatter(kept, dict(enumerate(sends, 1)), ("x", "y"))
    v = v.reshape(4, 224, 128)
    parts = {k: lax.dynamic_index_in_dim(v, (second + k) % 4, 0, keepdims=False) for k in range(4)}
    v = scatter(parts[0], parts, ("y", "x"))
    v = v + shifted(v, "zl", 2, 1)
    v = v.astype(bf16)
    got = {k: shifted(v, "zh", 4, k) for k in ORDER}
    v = ((v.astype(f32) + got[2].astype(f32)) + (got[1].astype(f32) + got[3].astype(f32))).astype(bf16)
    v = gather(v, ("y", "x"), second)
    v = gather(v, ("x", "y"), first).reshape(28, 128, 128)
    return v, shifted(v, "c", 2, 1)


def exchange(low, high, axis, size):
    up = [(i, i + 1) for i in range(size - 1)]
    down = [(i + 1, i) for i in range(size - 1)]
    return lax.ppermute(high, axis, up), lax.ppermute(low, axis, down)


def nt(a, k, kt, kw):
    w = jnp.concatenate([k[kt, kh, kw] for kh in range(3)], axis=1)
    return lax.dot_general(a, w, (((1,), (1,)), ((), ())), preferred_element_type=f32)


def slope(z, s):
    return s * (1.0 + z * (1.0 - s))


def rows(i, n):
    return pl.ds(pl.multiple_of(i * 32, 32), n)


def local_kernel(
    pos, xin, cot, sides, ends, k1, k2, vectors,
    own_out, send_out, d_out,
    line, x_all, a3, g3, g3own, d3own, a1t, a2t, acc, acc2,
):
    row0, col0, core = pos[0], pos[1], pos[2]
    bias1, scale1, shift1, scale2, shift2 = (vectors[i:i + 1, :] for i in range(5))
    line[...] = jnp.zeros_like(line)
    x_all[...] = jnp.zeros_like(x_all)
    g3own[...] = jnp.zeros_like(g3own)
    d3own[...] = jnp.zeros_like(d3own)

    def masks(first, n):
        q = lax.broadcasted_iota(jnp.int32, (n, 128), 0)
        col, row = (q >> 5) + first, q & 31
        own = (row >= 2) & (row < 25) & (col >= 2) & (col < 12)
        r, c = row + row0, col + col0
        inside = (r >= 0) & (r < 184) & (c >= 0) & (c < 320)
        return own, inside

    def spread(dst, t, first, n, order):
        for k, o in enumerate(order):
            dst[t, first:first + n, k * 128:(k + 1) * 128] = line[o:o + n, :].astype(bf16)

    def place(dst, base, which, main, t):
        for w in range(14):
            at = base + w * 32
            if 2 <= w < 12:
                dst[at + 2:at + 25, :] = main[t, w - 2].astype(f32)
            else:
                dst[at + 2:at + 25, :] = sides[w // 12, which, t, w % 12].astype(f32)
            dst[at:at + 2, :] = ends[0, which, t, w].astype(f32)
            dst[at + 25:at + 27, :] = ends[1, which, t, w].astype(f32)

    def enter(t, bias):
        own, inside = masks(0, 448)
        line[8:456, :] = jnp.zeros((448, 128), f32)
        place(line, 8, 1, cot, t)
        place(x_all, 0, 0, xin, t)
        spread(g3, t, 0, 448, (9, 8, 7))
        go = jnp.where(own, line[8:456, :], 0.0)
        line[8:456, :] = go
        spread(g3own, t, 0, 448, (9, 8, 7))
        z = x_all[...] * scale1 + shift1
        s = jax.nn.sigmoid(z)
        line[8:456, :] = jnp.where(inside, z * s, 0.0)
        spread(a3, t, 0, 448, (7, 8, 9))
        a1t[t] = jnp.transpose(line[40:552, :]).astype(bf16)
        return bias + jnp.sum(go.reshape(56, 8, 128), axis=0)

    bias_two = lax.fori_loop(0, 3, enter, jnp.zeros((8, 128), f32))

    for t in range(3):
        acc[t] = jnp.zeros((384, 128), f32)
        acc2[t] = jnp.zeros((384, 128), f32)

    def first_convs(kw, carry):
        for t in range(3):
            for kt in range(2 - t, 3):
                w = jnp.concatenate([k1[kt, kh, kw] for kh in range(3)], axis=0)
                acc[t] += jnp.dot(a3[t + kt - 2, rows(kw, 384), :], w, preferred_element_type=f32)
        for t in range(3):
            for kt in range(t, 3):
                acc2[t] += nt(g3[t - kt + 2, rows(2 - kw, 384), :], k2, kt, kw)
        return carry

    lax.fori_loop(0, 3, first_convs, 0)
    line[392:400, :] = jnp.zeros((8, 128), f32)

    def middle(t, bias):
        own, inside = masks(1, 384)
        z = (acc[t] + bias1) * scale2 + shift2
        s = jax.nn.sigmoid(z)
        line[8:392, :] = jnp.where(inside, z * s, 0.0)
        a2t[t] = jnp.transpose(line[8:520, :]).astype(bf16)
        d = jnp.where(inside, acc2[t] * slope(z, s) * scale2, 0.0)
        d = d.astype(bf16)
        d_out[t] = d
        do = jnp.where(own, d.astype(f32), 0.0)
        line[8:392, :] = do
        spread(d3own, t, 32, 384, (9, 8, 7))
        return bias + jnp.sum(do.reshape(48, 8, 128), axis=0)

    bias_one = lax.fori_loop(0, 3, middle, jnp.zeros((8, 128), f32))

    def put(b, value):
        half = (b >= 28).astype(jnp.int32)
        at = b - half * 28

        @pl.when(half == core)
        def _():
            own_out[at] = value

        @pl.when(half != core)
        def _():
            send_out[at] = value.astype(bf16)

    def second_convs(kw, carry):
        for base, field, cotan in ((0, a1t, d3own), (27, a2t, g3own)):
            for kt in range(3):
                part = None
                for t in range(2 - kt, 3):
                    term = jnp.dot(field[t + kt - 2], cotan[t, rows(2 - kw, 512), :], preferred_element_type=f32)
                    part = term if part is None else part + term
                for kh in range(3):
                    put(base + kt * 9 + kh * 3 + kw, part[:, kh * 128:(kh + 1) * 128])
        return carry

    lax.fori_loop(0, 3, second_convs, 0)

    extra = lax.broadcasted_iota(jnp.int32, (128, 128), 0)
    b1 = jnp.broadcast_to(jnp.sum(bias_one, axis=0, keepdims=True), (128, 128))
    b2 = jnp.broadcast_to(jnp.sum(bias_two, axis=0, keepdims=True), (128, 128))
    put(jnp.int32(54), jnp.where(extra < 8, b1, jnp.where(extra < 16, b2, 0.0)))
    put(jnp.int32(55), jnp.zeros((128, 128), f32))


def input_kernel(d, xin, cot, k1, vectors, gin, line, d3, acc):
    scale1, shift1 = vectors[1:2, :], vectors[2:3, :]
    line[...] = jnp.zeros_like(line)
    for t in range(3):
        acc[t] = jnp.zeros((320, 128), f32)
        line[8:392, :] = d[t].astype(f32)
        for k, o in enumerate((9, 8, 7)):
            d3[t, :, k * 128:(k + 1) * 128] = line[o:o + 384, :].astype(bf16)

    def convs(kw, carry):
        for t in range(3):
            for kt in range(t, 3):
                acc[t] += nt(d3[t - kt + 2, rows(2 - kw, 320), :], k1, kt, kw)
        return carry

    lax.fori_loop(0, 3, convs, 0)
    for t in range(3):
        for w in range(10):
            z = xin[t, w].astype(f32) * scale1 + shift1
            change = acc[t, w * 32 + 2:w * 32 + 25, :] * (slope(z, jax.nn.sigmoid(z)) * scale1)
            gin[t, w] = (cot[t, w].astype(f32) + change).astype(bf16)


def combine_kernel(pos, own, got, kept, to1, to2, to3):
    def one(j, carry):
        for k, out in enumerate((kept, to1, to2, to3)):
            b = lax.rem(pos[3] + k, 4) * 7 + j
            out[j] = (own[b] + got[b].astype(f32)).astype(out.dtype)
        return carry

    lax.fori_loop(0, 7, one, 0)


def final_kernel(pos, mine, other, one, two, bias_one, bias_two):
    factor = 1.0 / math.sqrt(CELLS)

    def emit(low, high):
        def block(b):
            ref, at = (low, b) if b < 28 else (high, b - 28)
            return ref[at].astype(f32) * factor

        for b in range(27):
            one[b] = block(b)
            two[b] = block(27 + b)
        bias_one[...] = high[26, 0:8, :].astype(f32) * factor
        bias_two[...] = high[26, 8:16, :].astype(f32) * factor

    @pl.when(pos[2] == 0)
    def _():
        emit(mine, other)

    @pl.when(pos[2] != 0)
    def _():
        emit(other, mine)


VMEM = pl.BlockSpec(memory_space=pltpu.VMEM)
SMEM = pl.BlockSpec(memory_space=pltpu.SMEM)


def call(kernel, out, inputs, scratch, mib, flops, size):
    return pl.pallas_call(
        kernel,
        out_shape=tuple(jax.ShapeDtypeStruct(*o) for o in out),
        in_specs=inputs,
        out_specs=(VMEM,) * len(out),
        scratch_shapes=scratch,
        compiler_params=pltpu.CompilerParams(vmem_limit_bytes=mib * 1024 * 1024),
        cost_estimate=pl.CostEstimate(flops=flops, bytes_accessed=size, transcendentals=0),
    )


def local(pos, xin, cot, sides, ends, k1, k2, vectors):
    return call(
        local_kernel,
        [((28, 128, 128), f32), ((28, 128, 128), bf16), ((3, 384, 128), bf16)],
        [SMEM] + [VMEM] * 7,
        [
            pltpu.VMEM((568, 128), f32),
            pltpu.VMEM((448, 128), f32),
            pltpu.VMEM((3, 448, 384), bf16),
            pltpu.VMEM((3, 448, 384), bf16),
            pltpu.VMEM((3, 576, 384), bf16),
            pltpu.VMEM((3, 576, 384), bf16),
            pltpu.VMEM((3, 128, 512), bf16),
            pltpu.VMEM((3, 128, 512), bf16),
            pltpu.VMEM((3, 384, 128), f32),
            pltpu.VMEM((3, 384, 128), f32),
        ],
        24, 4 * 10**9, 8 * 10**6,
    )(pos, xin, cot, sides, ends, k1, k2, vectors)


def input_grad(d, xin, cot, k1, vectors):
    return call(
        input_kernel,
        [((3, 10, 23, 128), bf16)],
        [VMEM] * 5,
        [
            pltpu.VMEM((400, 128), f32),
            pltpu.VMEM((3, 384, 384), bf16),
            pltpu.VMEM((3, 320, 128), f32),
        ],
        16, 10**9, 3 * 10**6,
    )(d, xin, cot, k1, vectors)[0]


def combine(pos, own, got):
    return call(
        combine_kernel, [((7, 128, 128), f32)] + [((7, 128, 128), bf16)] * 3, [SMEM, VMEM, VMEM], [],
        16, 10**6, 10**6,
    )(pos, own, got)


def final(pos, mine, other):
    shape = (27, 128, 128)
    return call(
        final_kernel, [(shape, f32), (shape, f32), ((8, 128), f32), ((8, 128), f32)], [SMEM, VMEM, VMEM], [],
        16, 10**6, 10**6,
    )(pos, mine, other)


def body(block_input, cotangent, kernel_one, bias_one, kernel_two, scale_one, shift_one, scale_two, shift_two):
    xin, cot = jnp.swapaxes(block_input, 1, 2), jnp.swapaxes(cotangent, 1, 2)
    low = jnp.stack([xin[:, :2], cot[:, :2]])
    high = jnp.stack([xin[:, 8:], cot[:, 8:]])
    left, right = exchange(low, high, "wa", 32)

    def edge(s):
        main = jnp.stack([xin[:, :, s], cot[:, :, s]])
        return jnp.concatenate([left[:, :, :, s], main, right[:, :, :, s]], axis=2)

    above, below = exchange(edge(slice(0, 2)), edge(slice(21, 23)), "ha", 8)
    ha, wa = lax.axis_index("ha"), lax.axis_index("wa")
    y, x, c = ha % 4, wa // 8, wa % 2
    first, second = jnp.where(c == 0, x, y), jnp.where(c == 0, y, x)
    pos = jnp.stack([ha * 23 - 2, wa * 10 - 2, c, first, second]).astype(jnp.int32)
    vectors = jnp.pad(jnp.stack([bias_one, scale_one, shift_one, scale_two, shift_two]), ((0, 3), (0, 0)))
    xin, cot, k1, k2 = (jnp.where(wa < 32, v, jnp.zeros_like(v)) for v in (xin, cot, kernel_one, kernel_two))
    own, send, d = local(pos, xin, cot, jnp.stack([left, right]), jnp.stack([above, below]), k1, k2, vectors)
    gin = input_grad(d, xin, cot, k1, vectors)
    grad_one, grad_two, grad_bias_one, grad_bias_two = final(pos, *total(pos, own, send))
    shape = (3, 3, 3, 128, 128)
    return (
        jnp.swapaxes(gin, 1, 2), grad_one.reshape(shape), grad_bias_one[0], grad_two.reshape(shape), grad_bias_two[0],
    )


def solution(mesh):
    split = P(None, "ha", "wa", None)
    return jax.shard_map(
        body,
        mesh=mesh,
        in_specs=(split, split) + (P(),) * 7,
        out_specs=(split,) + (P(),) * 4,
        check_vma=False,
    )
```

```python
import math

import jax
import jax.numpy as jnp
from jax import lax
from jax.experimental import pallas as pl
from jax.experimental.pallas import tpu as pltpu
from jax.sharding import PartitionSpec as P

CELLS = 176640
AXES = ("ha", "wa")
f32 = jnp.float32
bf16 = jnp.bfloat16


def coords(d):
    return {"zl": d // 128, "y": (d // 32) % 4, "x": (d // 8) % 4, "zh": (d // 2) % 4, "c": d % 2}


def device_of(p):
    return (((p["zl"] * 4 + p["y"]) * 4 + p["x"]) * 4 + p["zh"]) * 2 + p["c"]


def shift_pairs(axis, size, k):
    pairs = []
    for d in range(256):
        p = coords(d)
        a = axis if isinstance(axis, str) else axis[p["c"]]
        p[a] = (p[a] + k) % size
        pairs.append((d, device_of(p)))
    return pairs


def shifted(v, axis, size, k):
    return lax.ppermute(v, AXES, shift_pairs(axis, size, k))


ORDER = (2, 1, 3)


def scatter(own, send, axis):
    got = {k: shifted(send[k], axis, 4, k) for k in ORDER}
    return own + got[1].astype(f32) + got[2].astype(f32) + got[3].astype(f32)


def gather(v, axis, here):
    got = {k: shifted(v, axis, 4, k) for k in ORDER}
    out = lax.dynamic_update_index_in_dim(jnp.zeros((4,) + v.shape, v.dtype), v, here, 0)
    for k in (1, 3, 2):
        out = lax.dynamic_update_index_in_dim(out, got[k], (here - k) % 4, 0)
    return out


def total(pos, own, got):
    first, second = pos[3], pos[4]
    kept, *sends = combine(pos, own, got)
    v = scatter(kept, dict(enumerate(sends, 1)), ("x", "y"))
    v = v.reshape(4, 224, 128)
    parts = {k: lax.dynamic_index_in_dim(v, (second + k) % 4, 0, keepdims=False) for k in range(4)}
    v = scatter(parts[0], parts, ("y", "x"))
    v = v + shifted(v, "zl", 2, 1)
    v = v.astype(bf16)
    got = {k: shifted(v, "zh", 4, k) for k in ORDER}
    v = ((v.astype(f32) + got[2].astype(f32)) + (got[1].astype(f32) + got[3].astype(f32))).astype(bf16)
    v = gather(v, ("y", "x"), second)
    v = gather(v, ("x", "y"), first).reshape(28, 128, 128)
    return v, shifted(v, "c", 2, 1)


def exchange(low, high, axis, size):
    up = [(i, i + 1) for i in range(size - 1)]
    down = [(i + 1, i) for i in range(size - 1)]
    return lax.ppermute(high, axis, up), lax.ppermute(low, axis, down)


def adjoint(field, k, kw, acc, n):
    for s in range(3):
        w = jnp.concatenate(
            [jnp.concatenate([k[kt, kh, kw] for kh in range(3)], axis=1) for kt in range(2 - s, 3)], axis=0
        )
        part = lax.dot_general(
            field[s, rows(2 - kw, n), :], w, (((1,), (1,)), ((), ())), preferred_element_type=f32
        )
        for j, kt in enumerate(range(2 - s, 3)):
            acc[s - 2 + kt] += part[:, j * 128:(j + 1) * 128]


def slope(z, s):
    return s * (1.0 + z * (1.0 - s))


def rows(i, n):
    return pl.ds(pl.multiple_of(i * 32, 32), n)


def local_kernel(
    pos, xin, cot, sides, ends, k1, k2, vectors,
    send_out, bias_out, d_out, field, cotan,
    line, x_all, a3, g3, a2, acc, acc2,
):
    row0, col0, core = pos[0], pos[1], pos[2]
    bias1, scale1, shift1, scale2, shift2 = (vectors[i:i + 1, :] for i in range(5))
    line[...] = jnp.zeros_like(line)
    x_all[...] = jnp.zeros_like(x_all)
    for half in range(2):
        cotan[half, 960:1024, :] = jnp.zeros((64, 384), bf16)

    def masks(first, n):
        q = lax.broadcasted_iota(jnp.int32, (n, 128), 0)
        col, row = (q >> 5) + first, q & 31
        r, c = row + row0, col + col0
        inside = (r >= 0) & (r < 184) & (c >= 0) & (c < 320)
        return (row >= 2) & (row < 25), inside

    def place(dst, base, which, main, t):
        for w in range(14):
            at = base + w * 32
            if 2 <= w < 12:
                dst[at + 2:at + 25, :] = main[t, w - 2].astype(f32)
            else:
                dst[at + 2:at + 25, :] = sides[w // 12, which, t, w % 12].astype(f32)
            dst[at:at + 2, :] = ends[0, which, t, w].astype(f32)
            dst[at + 25:at + 27, :] = ends[1, which, t, w].astype(f32)

    def own_cells(half, t, first):
        at = pl.ds(pl.multiple_of(t * 320, 64), 320)
        for k, o in enumerate((9, 8, 7)):
            cotan[half, at, k * 128:(k + 1) * 128] = line[o + first:o + first + 320, :].astype(bf16)

    def enter(t, bias):
        own, inside = masks(0, 448)
        line[8:456, :] = jnp.zeros((448, 128), f32)
        place(line, 8, 1, cot, t)
        place(x_all, 0, 0, xin, t)
        for k, o in enumerate((9, 8, 7)):
            g3[t, :, k * 128:(k + 1) * 128] = line[o:o + 448, :].astype(bf16)
        go = jnp.where(own, line[8:456, :], 0.0)
        line[8:456, :] = go
        own_cells(1, t, 64)
        z = x_all[...] * scale1 + shift1
        line[8:456, :] = jnp.where(inside, z * jax.nn.sigmoid(z), 0.0)
        for k, o in enumerate((7, 8, 9)):
            a3[t, :, k * 128:(k + 1) * 128] = line[o:o + 448, :].astype(bf16)
        return bias + jnp.sum(go[64:384].reshape(40, 8, 128), axis=0)

    bias_two = lax.fori_loop(0, 3, enter, jnp.zeros((8, 128), f32))
    for t in range(3):
        acc[t] = jnp.zeros((384, 128), f32)
        acc2[t] = jnp.zeros((384, 128), f32)

    def first_convs(kw, carry):
        for s in range(3):
            w = jnp.concatenate(
                [jnp.concatenate([k1[kt, kh, kw] for kh in range(3)], axis=0) for kt in range(s, 3)], axis=1
            )
            part = jnp.dot(a3[s, rows(kw, 384), :], w, preferred_element_type=f32)
            for j, kt in enumerate(range(s, 3)):
                acc[s + 2 - kt] += part[:, j * 128:(j + 1) * 128]
        adjoint(g3, k2, kw, acc2, 384)
        return carry

    lax.fori_loop(0, 3, first_convs, 0)
    line[392:400, :] = jnp.zeros((8, 128), f32)

    def middle(t, bias):
        own, inside = masks(1, 384)
        z = (acc[t] + bias1) * scale2 + shift2
        s = jax.nn.sigmoid(z)
        a2[t] = jnp.where(inside, z * s, 0.0).astype(bf16)
        d = jnp.where(inside, acc2[t] * slope(z, s) * scale2, 0.0).astype(bf16)
        d_out[t] = d
        do = jnp.where(own, d.astype(f32), 0.0)
        line[8:392, :] = do
        own_cells(0, t, 32)
        return bias + jnp.sum(do[32:352].reshape(40, 8, 128), axis=0)

    bias_one = lax.fori_loop(0, 3, middle, jnp.zeros((8, 128), f32))
    tail = [jnp.zeros((64, 128), bf16)]
    for kw in range(3):
        at = slice(kw * 128, (kw + 1) * 128)
        first = [a3[t, (1 + kw) * 32:(1 + kw) * 32 + 320, 128:256] for t in range(3)]
        field[0, at, :] = jnp.transpose(jnp.concatenate(first + tail, axis=0))
        second = [a2[t, kw * 32:kw * 32 + 320, :] for t in range(3)]
        field[1, at, :] = jnp.transpose(jnp.concatenate(second + tail, axis=0))
    low = lax.broadcasted_iota(jnp.int32, (128, 128), 0)
    b1 = jnp.broadcast_to(jnp.sum(bias_one, axis=0, keepdims=True), (128, 128))
    b2 = jnp.broadcast_to(jnp.sum(bias_two, axis=0, keepdims=True), (128, 128))
    biases = jnp.where(low < 8, b1, jnp.where(low < 16, b2, 0.0))
    bias_out[...] = biases
    kernel_grads(field, cotan, 1 - core, biases, send_out)


def kernel_grads(field, cotan, half, biases, out):
    for kt, n in enumerate((384, 640, 1024)):
        start = (2 - kt) * 320
        part = jnp.dot(
            field[half, :, 0:n], cotan[half, start:start + n, :], preferred_element_type=f32
        ).astype(out.dtype)
        for kh in range(3):
            for kw in range(3):
                out[kt * 9 + kh * 3 + kw] = part[kw * 128:(kw + 1) * 128, kh * 128:(kh + 1) * 128]
    out[27] = jnp.where(half == 0, biases, 0.0).astype(out.dtype)


def own_kernel(pos, field, cotan, biases, out):
    kernel_grads(field, cotan, pos[2], biases[...], out)


def input_kernel(d, xin, cot, k1, vectors, gin, line, d3, acc):
    scale1, shift1 = vectors[1:2, :], vectors[2:3, :]
    line[...] = jnp.zeros_like(line)
    for t in range(3):
        acc[t] = jnp.zeros((320, 128), f32)
        line[8:392, :] = d[t].astype(f32)
        for k, o in enumerate((9, 8, 7)):
            d3[t, :, k * 128:(k + 1) * 128] = line[o:o + 384, :].astype(bf16)

    def convs(kw, carry):
        adjoint(d3, k1, kw, acc, 320)
        return carry

    lax.fori_loop(0, 3, convs, 0)
    for t in range(3):
        for w in range(10):
            z = xin[t, w].astype(f32) * scale1 + shift1
            change = acc[t, w * 32 + 2:w * 32 + 25, :] * (slope(z, jax.nn.sigmoid(z)) * scale1)
            gin[t, w] = (cot[t, w].astype(f32) + change).astype(bf16)


def combine_kernel(pos, own, got, kept, to1, to2, to3):
    def one(j, carry):
        for k, out in enumerate((kept, to1, to2, to3)):
            b = lax.rem(pos[3] + k, 4) * 7 + j
            out[j] = (own[b] + got[b].astype(f32)).astype(out.dtype)
        return carry

    lax.fori_loop(0, 7, one, 0)


PIECE = 9


def final_kernel(pos, mine, other, one, two, bias_one, bias_two, wide_one, wide_two, sems):
    factor = 1.0 / math.sqrt(CELLS)

    def emit(low, high):
        copies = []
        for p in range(0, 27, PIECE):
            for i, (src, wide, out) in enumerate(((low, wide_one, one), (high, wide_two, two))):
                wide[p:p + PIECE] = src[p:p + PIECE].astype(f32) * factor
                at = pl.ds(p, PIECE)
                copies.append(pltpu.make_async_copy(wide.at[at], out.at[at], sems.at[i, p // PIECE]))
                copies[-1].start()
        bias_one[...] = low[27, 0:1, :].astype(f32) * factor
        bias_two[...] = low[27, 8:9, :].astype(f32) * factor
        for copy in copies:
            copy.wait()

    @pl.when(pos[2] == 0)
    def _():
        emit(mine, other)

    @pl.when(pos[2] != 0)
    def _():
        emit(other, mine)


VMEM = pl.BlockSpec(memory_space=pltpu.VMEM)
HBM = pl.BlockSpec(memory_space=pltpu.HBM)
SMEM = pl.BlockSpec(memory_space=pltpu.SMEM)


def call(kernel, out, inputs, scratch, mib, flops, size, places=None):
    return pl.pallas_call(
        kernel,
        out_shape=tuple(jax.ShapeDtypeStruct(*o) for o in out),
        in_specs=inputs,
        out_specs=places or (VMEM,) * len(out),
        scratch_shapes=scratch,
        compiler_params=pltpu.CompilerParams(vmem_limit_bytes=mib * 1024 * 1024),
        cost_estimate=pl.CostEstimate(flops=flops, bytes_accessed=size, transcendentals=0),
    )


def local(pos, xin, cot, sides, ends, k1, k2, vectors):
    return call(
        local_kernel,
        [
            ((28, 128, 128), bf16), ((128, 128), f32), ((3, 384, 128), bf16),
            ((2, 384, 1024), bf16), ((2, 1024, 384), bf16),
        ],
        [SMEM] + [VMEM] * 7,
        [
            pltpu.VMEM((464, 128), f32),
            pltpu.VMEM((448, 128), f32),
            pltpu.VMEM((3, 448, 384), bf16),
            pltpu.VMEM((3, 448, 384), bf16),
            pltpu.VMEM((3, 384, 128), bf16),
            pltpu.VMEM((3, 384, 128), f32),
            pltpu.VMEM((3, 384, 128), f32),
        ],
        24, 3 * 10**9, 8 * 10**6,
    )(pos, xin, cot, sides, ends, k1, k2, vectors)


def own_grads(pos, field, cotan, biases):
    return call(
        own_kernel, [((28, 128, 128), f32)], [SMEM, VMEM, VMEM, VMEM], [], 16, 10**9, 3 * 10**6,
    )(pos, field, cotan, biases)[0]


def input_grad(d, xin, cot, k1, vectors):
    return call(
        input_kernel,
        [((3, 10, 23, 128), bf16)],
        [VMEM] * 5,
        [
            pltpu.VMEM((400, 128), f32),
            pltpu.VMEM((3, 384, 384), bf16),
            pltpu.VMEM((3, 320, 128), f32),
        ],
        16, 10**9, 3 * 10**6,
    )(d, xin, cot, k1, vectors)[0]


def combine(pos, own, got):
    return call(
        combine_kernel, [((7, 128, 128), f32)] + [((7, 128, 128), bf16)] * 3, [SMEM, VMEM, VMEM], [],
        16, 10**6, 10**6,
    )(pos, own, got)


def final(pos, mine, other):
    shape = (27, 128, 128)
    return call(
        final_kernel, [(shape, f32), (shape, f32), ((1, 128), f32), ((1, 128), f32)], [SMEM, VMEM, VMEM],
        [pltpu.VMEM(shape, f32), pltpu.VMEM(shape, f32), pltpu.SemaphoreType.DMA((2, 3))],
        56, 10**6, 10**6, (HBM, HBM, VMEM, VMEM),
    )(pos, mine, other)


def body(block_input, cotangent, kernel_one, bias_one, kernel_two, scale_one, shift_one, scale_two, shift_two):
    xin, cot = jnp.swapaxes(block_input, 1, 2), jnp.swapaxes(cotangent, 1, 2)
    low = jnp.stack([xin[:, :2], cot[:, :2]])
    high = jnp.stack([xin[:, 8:], cot[:, 8:]])
    left, right = exchange(low, high, "wa", 32)

    def edge(s):
        main = jnp.stack([xin[:, :, s], cot[:, :, s]])
        return jnp.concatenate([left[:, :, :, s], main, right[:, :, :, s]], axis=2)

    above, below = exchange(edge(slice(0, 2)), edge(slice(21, 23)), "ha", 8)
    ha, wa = lax.axis_index("ha"), lax.axis_index("wa")
    y, x, c = ha % 4, wa // 8, wa % 2
    first, second = jnp.where(c == 0, x, y), jnp.where(c == 0, y, x)
    pos = jnp.stack([ha * 23 - 2, wa * 10 - 2, c, first, second]).astype(jnp.int32)
    vectors = jnp.pad(jnp.stack([bias_one, scale_one, shift_one, scale_two, shift_two]), ((0, 3), (0, 0)))
    xin, cot, k1, k2 = (jnp.where(wa < 32, v, jnp.zeros_like(v)) for v in (xin, cot, kernel_one, kernel_two))
    send, biases, d, field, cotan = local(pos, xin, cot, jnp.stack([left, right]), jnp.stack([above, below]), k1, k2, vectors)
    got = shifted(send, "c", 2, 1)
    own = own_grads(pos, field, cotan, biases)
    gin = input_grad(d, xin, cot, k1, vectors)
    grad_one, grad_two, grad_bias_one, grad_bias_two = final(pos, *total(pos, own, got))
    shape = (3, 3, 3, 128, 128)
    return (
        jnp.swapaxes(gin, 1, 2), grad_one.reshape(shape), grad_bias_one[0], grad_two.reshape(shape), grad_bias_two[0],
    )


def solution(mesh):
    split = P(None, "ha", "wa", None)
    return jax.shard_map(
        body,
        mesh=mesh,
        in_specs=(split, split) + (P(),) * 7,
        out_specs=(split,) + (P(),) * 4,
        check_vma=False,
    )
```

```python
import math

import jax
import jax.numpy as jnp
from jax import lax
from jax.experimental import pallas as pl
from jax.experimental.pallas import tpu as pltpu
from jax.sharding import PartitionSpec as P

CELLS = 176640
AXES = ("ha", "wa")
f32 = jnp.float32
bf16 = jnp.bfloat16


def coords(d):
    return {"zl": d // 128, "y": (d // 32) % 4, "x": (d // 8) % 4, "zh": (d // 2) % 4, "c": d % 2}


def device_of(p):
    return (((p["zl"] * 4 + p["y"]) * 4 + p["x"]) * 4 + p["zh"]) * 2 + p["c"]


def shift_pairs(axis, size, k):
    pairs = []
    for d in range(256):
        p = coords(d)
        a = axis if isinstance(axis, str) else axis[p["c"]]
        p[a] = (p[a] + k) % size
        pairs.append((d, device_of(p)))
    return pairs


def shifted(v, axis, size, k):
    return lax.ppermute(v, AXES, shift_pairs(axis, size, k))


ORDER = (2, 1, 3)


def scatter(send, axis):
    got = {k: shifted(send[k - 1], axis, 4, k) for k in ORDER}
    return got[1], got[2], got[3]


def gather(v, axis, here):
    got = {k: shifted(v, axis, 4, k) for k in ORDER}
    out = lax.dynamic_update_index_in_dim(jnp.zeros((4,) + v.shape, v.dtype), v, here, 0)
    for k in (1, 3, 2):
        out = lax.dynamic_update_index_in_dim(out, got[k], (here - k) % 4, 0)
    return out


def total(pos, own, got):
    first, second = pos[3], pos[4]
    kept, *sends = combine(pos, own, got)
    kept, *sends = fold(pos, kept, scatter(sends, ("x", "y")))
    got = scatter(sends, ("y", "x"))
    v = kept + got[0].astype(f32) + got[1].astype(f32) + got[2].astype(f32)
    v = v + shifted(v, "zl", 2, 1)
    v = v.astype(bf16)
    got = {k: shifted(v, "zh", 4, k) for k in ORDER}
    v = ((v.astype(f32) + got[2].astype(f32)) + (got[1].astype(f32) + got[3].astype(f32))).astype(bf16)
    v = gather(v, ("y", "x"), second)
    v = gather(v, ("x", "y"), first).reshape(28, 128, 128)
    other = shifted(v, "c", 2, 1)
    one, two = write_mine(pos, v)
    return write_other(pos, v, other, one, two)


def exchange(low, high, axis, size):
    up = [(i, i + 1) for i in range(size - 1)]
    down = [(i + 1, i) for i in range(size - 1)]
    return lax.ppermute(high, axis, up), lax.ppermute(low, axis, down)


def adjoint(field, k, kw, acc, n):
    for s in range(3):
        w = jnp.concatenate(
            [jnp.concatenate([k[kt, kh, kw] for kh in range(3)], axis=1) for kt in range(2 - s, 3)], axis=0
        )
        part = lax.dot_general(
            field[s, rows(2 - kw, n), :], w, (((1,), (1,)), ((), ())), preferred_element_type=f32
        )
        for j, kt in enumerate(range(2 - s, 3)):
            acc[s - 2 + kt] += part[:, j * 128:(j + 1) * 128]


def slope(z, s):
    return s * (1.0 + z * (1.0 - s))


def rows(i, n):
    return pl.ds(pl.multiple_of(i * 32, 32), n)


def local_kernel(
    pos, xin, cot, sides, ends, k1, k2, vectors,
    send_out, bias_out, d_out, field, cotan,
    line, x_all, a3, g3, a2, acc, acc2,
):
    row0, col0, core = pos[0], pos[1], pos[2]
    bias1, scale1, shift1, scale2, shift2 = (vectors[i:i + 1, :] for i in range(5))
    line[...] = jnp.zeros_like(line)
    x_all[...] = jnp.zeros_like(x_all)
    for half in range(2):
        cotan[half, 960:1024, :] = jnp.zeros((64, 384), bf16)

    def masks(first, n):
        q = lax.broadcasted_iota(jnp.int32, (n, 128), 0)
        col, row = (q >> 5) + first, q & 31
        r, c = row + row0, col + col0
        inside = (r >= 0) & (r < 184) & (c >= 0) & (c < 320)
        return (row >= 2) & (row < 25), inside

    def place(dst, base, which, main, t):
        for w in range(14):
            at = base + w * 32
            if 2 <= w < 12:
                dst[at + 2:at + 25, :] = main[t, w - 2].astype(f32)
            else:
                dst[at + 2:at + 25, :] = sides[w // 12, which, t, w % 12].astype(f32)
            dst[at:at + 2, :] = ends[0, which, t, w].astype(f32)
            dst[at + 25:at + 27, :] = ends[1, which, t, w].astype(f32)

    def own_cells(half, t, first):
        at = pl.ds(pl.multiple_of(t * 320, 64), 320)
        for k, o in enumerate((9, 8, 7)):
            cotan[half, at, k * 128:(k + 1) * 128] = line[o + first:o + first + 320, :].astype(bf16)

    def enter(t, bias):
        own, inside = masks(0, 448)
        line[8:456, :] = jnp.zeros((448, 128), f32)
        place(line, 8, 1, cot, t)
        place(x_all, 0, 0, xin, t)
        for k, o in enumerate((9, 8, 7)):
            g3[t, :, k * 128:(k + 1) * 128] = line[o:o + 448, :].astype(bf16)
        go = jnp.where(own, line[8:456, :], 0.0)
        line[8:456, :] = go
        own_cells(1, t, 64)
        z = x_all[...] * scale1 + shift1
        line[8:456, :] = jnp.where(inside, z * jax.nn.sigmoid(z), 0.0)
        for k, o in enumerate((7, 8, 9)):
            a3[t, :, k * 128:(k + 1) * 128] = line[o:o + 448, :].astype(bf16)
        return bias + jnp.sum(go[64:384].reshape(40, 8, 128), axis=0)

    bias_two = lax.fori_loop(0, 3, enter, jnp.zeros((8, 128), f32))
    for t in range(3):
        acc[t] = jnp.zeros((384, 128), f32)
        acc2[t] = jnp.zeros((384, 128), f32)

    def first_convs(kw, carry):
        for s in range(3):
            w = jnp.concatenate(
                [jnp.concatenate([k1[kt, kh, kw] for kh in range(3)], axis=0) for kt in range(s, 3)], axis=1
            )
            part = jnp.dot(a3[s, rows(kw, 384), :], w, preferred_element_type=f32)
            for j, kt in enumerate(range(s, 3)):
                acc[s + 2 - kt] += part[:, j * 128:(j + 1) * 128]
        adjoint(g3, k2, kw, acc2, 384)
        return carry

    lax.fori_loop(0, 3, first_convs, 0)
    line[392:400, :] = jnp.zeros((8, 128), f32)

    def middle(t, bias):
        own, inside = masks(1, 384)
        z = (acc[t] + bias1) * scale2 + shift2
        s = jax.nn.sigmoid(z)
        a2[t] = jnp.where(inside, z * s, 0.0).astype(bf16)
        d = jnp.where(inside, acc2[t] * slope(z, s) * scale2, 0.0).astype(bf16)
        d_out[t] = d
        do = jnp.where(own, d.astype(f32), 0.0)
        line[8:392, :] = do
        own_cells(0, t, 32)
        return bias + jnp.sum(do[32:352].reshape(40, 8, 128), axis=0)

    bias_one = lax.fori_loop(0, 3, middle, jnp.zeros((8, 128), f32))
    tail = [jnp.zeros((64, 128), bf16)]
    for kw in range(3):
        at = slice(kw * 128, (kw + 1) * 128)
        first = [a3[t, (1 + kw) * 32:(1 + kw) * 32 + 320, 128:256] for t in range(3)]
        field[0, at, :] = jnp.transpose(jnp.concatenate(first + tail, axis=0))
        second = [a2[t, kw * 32:kw * 32 + 320, :] for t in range(3)]
        field[1, at, :] = jnp.transpose(jnp.concatenate(second + tail, axis=0))
    low = lax.broadcasted_iota(jnp.int32, (128, 128), 0)
    b1 = jnp.broadcast_to(jnp.sum(bias_one, axis=0, keepdims=True), (128, 128))
    b2 = jnp.broadcast_to(jnp.sum(bias_two, axis=0, keepdims=True), (128, 128))
    biases = jnp.where(low < 8, b1, jnp.where(low < 16, b2, 0.0))
    bias_out[...] = biases
    kernel_grads(field, cotan, 1 - core, biases, send_out)


def kernel_grads(field, cotan, half, biases, out):
    for kt, n in enumerate((384, 640, 1024)):
        start = (2 - kt) * 320
        part = jnp.dot(
            field[half, :, 0:n], cotan[half, start:start + n, :], preferred_element_type=f32
        ).astype(out.dtype)
        for kh in range(3):
            for kw in range(3):
                out[kt * 9 + kh * 3 + kw] = part[kw * 128:(kw + 1) * 128, kh * 128:(kh + 1) * 128]
    out[27] = jnp.where(half == 0, biases, 0.0).astype(out.dtype)


def own_kernel(pos, field, cotan, biases, out):
    kernel_grads(field, cotan, pos[2], biases[...], out)


def input_kernel(d, xin, cot, k1, vectors, gin, line, d3, acc):
    scale1, shift1 = vectors[1:2, :], vectors[2:3, :]
    line[...] = jnp.zeros_like(line)
    for t in range(3):
        acc[t] = jnp.zeros((320, 128), f32)
        line[8:392, :] = d[t].astype(f32)
        for k, o in enumerate((9, 8, 7)):
            d3[t, :, k * 128:(k + 1) * 128] = line[o:o + 384, :].astype(bf16)

    def convs(kw, carry):
        adjoint(d3, k1, kw, acc, 320)
        return carry

    lax.fori_loop(0, 3, convs, 0)
    for t in range(3):
        for w in range(10):
            z = xin[t, w].astype(f32) * scale1 + shift1
            change = acc[t, w * 32 + 2:w * 32 + 25, :] * (slope(z, jax.nn.sigmoid(z)) * scale1)
            gin[t, w] = (cot[t, w].astype(f32) + change).astype(bf16)


def combine_kernel(pos, own, got, kept, to1, to2, to3):
    def one(j, carry):
        for k, out in enumerate((kept, to1, to2, to3)):
            b = lax.rem(pos[3] + k, 4) * 7 + j
            out[j] = (own[b] + got[b].astype(f32)).astype(out.dtype)
        return carry

    lax.fori_loop(0, 7, one, 0)


def fold_kernel(pos, own, got1, got2, got3, kept, to1, to2, to3):
    for k, out in enumerate((kept, to1, to2, to3)):
        at = lax.rem(pos[4] + k, 4)
        value = own[at] + got1[at].astype(f32) + got2[at].astype(f32) + got3[at].astype(f32)
        out[...] = value.astype(out.dtype)


FACTOR = 1.0 / math.sqrt(CELLS)
PIECE = 9


def write_half(half, src, one, two, wide, sems):
    def emit(out):
        copies = []
        for p in range(0, 27, PIECE):
            wide[p:p + PIECE] = src[p:p + PIECE].astype(f32) * FACTOR
            at = pl.ds(p, PIECE)
            copies.append(pltpu.make_async_copy(wide.at[at], out.at[at], sems.at[p // PIECE]))
            copies[-1].start()
        for copy in copies:
            copy.wait()

    @pl.when(half == 0)
    def _():
        emit(one)

    @pl.when(half != 0)
    def _():
        emit(two)


def mine_kernel(pos, mine, one, two, wide, sems):
    write_half(pos[2], mine, one, two, wide, sems)


def other_kernel(pos, mine, other, one_in, two_in, one, two, bias_one, bias_two, wide, sems):
    def biases(src):
        bias_one[...] = src[27, 0:1, :].astype(f32) * FACTOR
        bias_two[...] = src[27, 8:9, :].astype(f32) * FACTOR

    @pl.when(pos[2] == 0)
    def _():
        biases(mine)

    @pl.when(pos[2] != 0)
    def _():
        biases(other)

    write_half(1 - pos[2], other, one, two, wide, sems)


VMEM = pl.BlockSpec(memory_space=pltpu.VMEM)
HBM = pl.BlockSpec(memory_space=pltpu.HBM)
SMEM = pl.BlockSpec(memory_space=pltpu.SMEM)


def call(kernel, out, inputs, scratch, mib, flops, size, places=None, aliases=None):
    return pl.pallas_call(
        kernel,
        out_shape=tuple(jax.ShapeDtypeStruct(*o) for o in out),
        in_specs=inputs,
        out_specs=places or (VMEM,) * len(out),
        scratch_shapes=scratch,
        input_output_aliases=aliases or {},
        compiler_params=pltpu.CompilerParams(vmem_limit_bytes=mib * 1024 * 1024),
        cost_estimate=pl.CostEstimate(flops=flops, bytes_accessed=size, transcendentals=0),
    )


def local(pos, xin, cot, sides, ends, k1, k2, vectors):
    return call(
        local_kernel,
        [
            ((28, 128, 128), bf16), ((128, 128), f32), ((3, 384, 128), bf16),
            ((2, 384, 1024), bf16), ((2, 1024, 384), bf16),
        ],
        [SMEM] + [VMEM] * 7,
        [
            pltpu.VMEM((464, 128), f32),
            pltpu.VMEM((448, 128), f32),
            pltpu.VMEM((3, 448, 384), bf16),
            pltpu.VMEM((3, 448, 384), bf16),
            pltpu.VMEM((3, 384, 128), bf16),
            pltpu.VMEM((3, 384, 128), f32),
            pltpu.VMEM((3, 384, 128), f32),
        ],
        24, 3 * 10**9, 8 * 10**6,
    )(pos, xin, cot, sides, ends, k1, k2, vectors)


def own_grads(pos, field, cotan, biases):
    return call(
        own_kernel, [((28, 128, 128), f32)], [SMEM, VMEM, VMEM, VMEM], [], 16, 10**9, 3 * 10**6,
    )(pos, field, cotan, biases)[0]


def input_grad(d, xin, cot, k1, vectors):
    return call(
        input_kernel,
        [((3, 10, 23, 128), bf16)],
        [VMEM] * 5,
        [
            pltpu.VMEM((400, 128), f32),
            pltpu.VMEM((3, 384, 384), bf16),
            pltpu.VMEM((3, 320, 128), f32),
        ],
        16, 10**9, 3 * 10**6,
    )(d, xin, cot, k1, vectors)[0]


def combine(pos, own, got):
    return call(
        combine_kernel, [((7, 128, 128), f32)] + [((7, 128, 128), bf16)] * 3, [SMEM, VMEM, VMEM], [],
        16, 10**6, 10**6,
    )(pos, own, got)


def fold(pos, kept, got):
    parts = [v.reshape(4, 224, 128) for v in (kept, *got)]
    return call(
        fold_kernel, [((224, 128), f32)] + [((224, 128), bf16)] * 3, [SMEM] + [VMEM] * 4, [], 8, 10**6, 10**6,
    )(pos, *parts)


GRAD = ((27, 128, 128), f32)


def write_mine(pos, mine):
    return call(
        mine_kernel, [GRAD, GRAD], [SMEM, VMEM],
        [pltpu.VMEM(*GRAD), pltpu.SemaphoreType.DMA((3,))],
        8, 10**8, 10**6, (HBM, HBM),
    )(pos, mine)


def write_other(pos, mine, other, one, two):
    bias = ((1, 128), f32)
    return call(
        other_kernel, [GRAD, GRAD, bias, bias], [SMEM, VMEM, VMEM, HBM, HBM],
        [pltpu.VMEM(*GRAD), pltpu.SemaphoreType.DMA((3,))],
        8, 10**6, 10**6, (HBM, HBM, VMEM, VMEM), {3: 0, 4: 1},
    )(pos, mine, other, one, two)


def body(block_input, cotangent, kernel_one, bias_one, kernel_two, scale_one, shift_one, scale_two, shift_two):
    xin, cot = jnp.swapaxes(block_input, 1, 2), jnp.swapaxes(cotangent, 1, 2)
    low = jnp.stack([xin[:, :2], cot[:, :2]])
    high = jnp.stack([xin[:, 8:], cot[:, 8:]])
    left, right = exchange(low, high, "wa", 32)

    def edge(s):
        main = jnp.stack([xin[:, :, s], cot[:, :, s]])
        return jnp.concatenate([left[:, :, :, s], main, right[:, :, :, s]], axis=2)

    above, below = exchange(edge(slice(0, 2)), edge(slice(21, 23)), "ha", 8)
    ha, wa = lax.axis_index("ha"), lax.axis_index("wa")
    y, x, c = ha % 4, wa // 8, wa % 2
    first, second = jnp.where(c == 0, x, y), jnp.where(c == 0, y, x)
    pos = jnp.stack([ha * 23 - 2, wa * 10 - 2, c, first, second]).astype(jnp.int32)
    vectors = jnp.pad(jnp.stack([bias_one, scale_one, shift_one, scale_two, shift_two]), ((0, 3), (0, 0)))
    xin, cot, k1, k2 = (jnp.where(wa < 32, v, jnp.zeros_like(v)) for v in (xin, cot, kernel_one, kernel_two))
    send, biases, d, field, cotan = local(pos, xin, cot, jnp.stack([left, right]), jnp.stack([above, below]), k1, k2, vectors)
    got = shifted(send, "c", 2, 1)
    own = own_grads(pos, field, cotan, biases)
    gin = input_grad(d, xin, cot, k1, vectors)
    grad_one, grad_two, grad_bias_one, grad_bias_two = total(pos, own, got)
    shape = (3, 3, 3, 128, 128)
    return (
        jnp.swapaxes(gin, 1, 2), grad_one.reshape(shape), grad_bias_one[0], grad_two.reshape(shape), grad_bias_two[0],
    )


def solution(mesh):
    split = P(None, "ha", "wa", None)
    return jax.shard_map(
        body,
        mesh=mesh,
        in_specs=(split, split) + (P(),) * 7,
        out_specs=(split,) + (P(),) * 4,
        check_vma=False,
    )
```

```python
import math

import jax
import jax.numpy as jnp
from jax import lax
from jax.experimental import pallas as pl
from jax.experimental.pallas import tpu as pltpu
from jax.sharding import PartitionSpec as P

CELLS = 176640
AXES = ("ha", "wa")
f32 = jnp.float32
bf16 = jnp.bfloat16


def coords(d):
    return {"zl": d // 128, "y": (d // 32) % 4, "x": (d // 8) % 4, "zh": (d // 2) % 4, "c": d % 2}


def device_of(p):
    return (((p["zl"] * 4 + p["y"]) * 4 + p["x"]) * 4 + p["zh"]) * 2 + p["c"]


def shift_pairs(axis, size, k):
    pairs = []
    for d in range(256):
        p = coords(d)
        p[axis] = (p[axis] + k) % size
        pairs.append((d, device_of(p)))
    return pairs


def place(v, flip):
    return (v >> 1) ^ (v & 1) if flip == 1 else v >> 1


def position(x, y, flip):
    return place(x, flip) + 2 * place(y, flip)


def flip_pairs(flips, m):
    pairs = []
    for d in range(256):
        p = coords(d)
        p["x"] ^= flips[p["c"]] * (m & 1)
        p["y"] ^= flips[p["c"]] * (m >> 1)
        pairs.append((d, device_of(p)))
    return pairs


def send_pairs(v, pairs):
    return lax.ppermute(v, AXES, pairs)


def shifted(v, axis, size, k):
    return send_pairs(v, shift_pairs(axis, size, k))


def exchange_squares(sends, flips):
    return [send_pairs(sends[m - 1], flip_pairs(flips, m)) for m in (1, 2, 3)]


def gather(v, flips, here):
    got = exchange_squares([v] * 3, flips)
    out = lax.dynamic_update_index_in_dim(jnp.zeros((4,) + v.shape, v.dtype), v, here, 0)
    for m in (2, 1, 3):
        out = lax.dynamic_update_index_in_dim(out, got[m - 1], here ^ m, 0)
    return out


FIRST, SECOND = (1, 3), (3, 1)


def total(pos, own, got):
    first, second = pos[3], pos[4]
    kept, *sends = combine(pos, own, got)
    kept, *sends = fold(pos, kept, exchange_squares(sends, FIRST))
    got = exchange_squares(sends, SECOND)
    v = kept + got[0].astype(f32) + got[1].astype(f32) + got[2].astype(f32)
    v = v + shifted(v, "zl", 2, 1)
    v = v.astype(bf16)
    got = {k: shifted(v, "zh", 4, k) for k in (1, 2, 3)}
    v = ((v.astype(f32) + got[2].astype(f32)) + (got[1].astype(f32) + got[3].astype(f32))).astype(bf16)
    v = gather(v, SECOND, second)
    v = gather(v, FIRST, first).reshape(28, 128, 128)
    other = shifted(v, "c", 2, 1)
    one, two = write_mine(pos, v)
    return write_other(pos, v, other, one, two)


def exchange(low, high, axis, size):
    up = [(i, i + 1) for i in range(size - 1)]
    down = [(i + 1, i) for i in range(size - 1)]
    return lax.ppermute(high, axis, up), lax.ppermute(low, axis, down)


def adjoint(field, k, kw, acc, n):
    for s in range(3):
        w = jnp.concatenate(
            [jnp.concatenate([k[kt, kh, kw] for kh in range(3)], axis=1) for kt in range(2 - s, 3)], axis=0
        )
        part = lax.dot_general(
            field[s, rows(2 - kw, n), :], w, (((1,), (1,)), ((), ())), preferred_element_type=f32
        )
        for j, kt in enumerate(range(2 - s, 3)):
            acc[s - 2 + kt] += part[:, j * 128:(j + 1) * 128]


def slope(z, s):
    return s * (1.0 + z * (1.0 - s))


def rows(i, n):
    return pl.ds(pl.multiple_of(i * 32, 32), n)


def local_kernel(
    pos, xin, cot, sides, ends, k1, k2, vectors,
    send_out, bias_out, d_out, field, cotan,
    line, x_all, a3, g3, a2, acc, acc2,
):
    row0, col0, core = pos[0], pos[1], pos[2]
    bias1, scale1, shift1, scale2, shift2 = (vectors[i:i + 1, :] for i in range(5))
    line[...] = jnp.zeros_like(line)
    x_all[...] = jnp.zeros_like(x_all)
    for half in range(2):
        cotan[half, 960:1024, :] = jnp.zeros((64, 384), bf16)

    def masks(first, n):
        q = lax.broadcasted_iota(jnp.int32, (n, 128), 0)
        col, row = (q >> 5) + first, q & 31
        r, c = row + row0, col + col0
        inside = (r >= 0) & (r < 184) & (c >= 0) & (c < 320)
        return (row >= 2) & (row < 25), inside

    def place(dst, base, which, main, t):
        for w in range(14):
            at = base + w * 32
            if 2 <= w < 12:
                dst[at + 2:at + 25, :] = main[t, w - 2].astype(f32)
            else:
                dst[at + 2:at + 25, :] = sides[w // 12, which, t, w % 12].astype(f32)
            dst[at:at + 2, :] = ends[0, which, t, w].astype(f32)
            dst[at + 25:at + 27, :] = ends[1, which, t, w].astype(f32)

    def own_cells(half, t, first):
        at = pl.ds(pl.multiple_of(t * 320, 64), 320)
        for k, o in enumerate((9, 8, 7)):
            cotan[half, at, k * 128:(k + 1) * 128] = line[o + first:o + first + 320, :].astype(bf16)

    def enter(t, bias):
        own, inside = masks(0, 448)
        line[8:456, :] = jnp.zeros((448, 128), f32)
        place(line, 8, 1, cot, t)
        place(x_all, 0, 0, xin, t)
        for k, o in enumerate((9, 8, 7)):
            g3[t, :, k * 128:(k + 1) * 128] = line[o:o + 448, :].astype(bf16)
        go = jnp.where(own, line[8:456, :], 0.0)
        line[8:456, :] = go
        own_cells(1, t, 64)
        z = x_all[...] * scale1 + shift1
        line[8:456, :] = jnp.where(inside, z * jax.nn.sigmoid(z), 0.0)
        for k, o in enumerate((7, 8, 9)):
            a3[t, :, k * 128:(k + 1) * 128] = line[o:o + 448, :].astype(bf16)
        return bias + jnp.sum(go[64:384].reshape(40, 8, 128), axis=0)

    bias_two = lax.fori_loop(0, 3, enter, jnp.zeros((8, 128), f32))
    for t in range(3):
        acc[t] = jnp.zeros((384, 128), f32)
        acc2[t] = jnp.zeros((384, 128), f32)

    def first_convs(kw, carry):
        for s in range(3):
            w = jnp.concatenate(
                [jnp.concatenate([k1[kt, kh, kw] for kh in range(3)], axis=0) for kt in range(s, 3)], axis=1
            )
            part = jnp.dot(a3[s, rows(kw, 384), :], w, preferred_element_type=f32)
            for j, kt in enumerate(range(s, 3)):
                acc[s + 2 - kt] += part[:, j * 128:(j + 1) * 128]
        adjoint(g3, k2, kw, acc2, 384)
        return carry

    lax.fori_loop(0, 3, first_convs, 0)
    line[392:400, :] = jnp.zeros((8, 128), f32)

    def middle(t, bias):
        own, inside = masks(1, 384)
        z = (acc[t] + bias1) * scale2 + shift2
        s = jax.nn.sigmoid(z)
        a2[t] = jnp.where(inside, z * s, 0.0).astype(bf16)
        d = jnp.where(inside, acc2[t] * slope(z, s) * scale2, 0.0).astype(bf16)
        d_out[t] = d
        do = jnp.where(own, d.astype(f32), 0.0)
        line[8:392, :] = do
        own_cells(0, t, 32)
        return bias + jnp.sum(do[32:352].reshape(40, 8, 128), axis=0)

    bias_one = lax.fori_loop(0, 3, middle, jnp.zeros((8, 128), f32))
    tail = [jnp.zeros((64, 128), bf16)]
    for kw in range(3):
        at = slice(kw * 128, (kw + 1) * 128)
        first = [a3[t, (1 + kw) * 32:(1 + kw) * 32 + 320, 128:256] for t in range(3)]
        field[0, at, :] = jnp.transpose(jnp.concatenate(first + tail, axis=0))
        second = [a2[t, kw * 32:kw * 32 + 320, :] for t in range(3)]
        field[1, at, :] = jnp.transpose(jnp.concatenate(second + tail, axis=0))
    low = lax.broadcasted_iota(jnp.int32, (128, 128), 0)
    b1 = jnp.broadcast_to(jnp.sum(bias_one, axis=0, keepdims=True), (128, 128))
    b2 = jnp.broadcast_to(jnp.sum(bias_two, axis=0, keepdims=True), (128, 128))
    biases = jnp.where(low < 8, b1, jnp.where(low < 16, b2, 0.0))
    bias_out[...] = biases
    kernel_grads(field, cotan, 1 - core, biases, send_out)


def kernel_grads(field, cotan, half, biases, out):
    for kt, n in enumerate((384, 640, 1024)):
        start = (2 - kt) * 320
        part = jnp.dot(
            field[half, :, 0:n], cotan[half, start:start + n, :], preferred_element_type=f32
        ).astype(out.dtype)
        for kh in range(3):
            for kw in range(3):
                out[kt * 9 + kh * 3 + kw] = part[kw * 128:(kw + 1) * 128, kh * 128:(kh + 1) * 128]
    out[27] = jnp.where(half == 0, biases, 0.0).astype(out.dtype)


def own_kernel(pos, field, cotan, biases, out):
    kernel_grads(field, cotan, pos[2], biases[...], out)


def input_kernel(d, xin, cot, k1, vectors, gin, line, d3, acc):
    scale1, shift1 = vectors[1:2, :], vectors[2:3, :]
    line[...] = jnp.zeros_like(line)
    for t in range(3):
        acc[t] = jnp.zeros((320, 128), f32)
        line[8:392, :] = d[t].astype(f32)
        for k, o in enumerate((9, 8, 7)):
            d3[t, :, k * 128:(k + 1) * 128] = line[o:o + 384, :].astype(bf16)

    def convs(kw, carry):
        adjoint(d3, k1, kw, acc, 320)
        return carry

    lax.fori_loop(0, 3, convs, 0)
    for t in range(3):
        for w in range(10):
            z = xin[t, w].astype(f32) * scale1 + shift1
            change = acc[t, w * 32 + 2:w * 32 + 25, :] * (slope(z, jax.nn.sigmoid(z)) * scale1)
            gin[t, w] = (cot[t, w].astype(f32) + change).astype(bf16)


def combine_kernel(pos, own, got, kept, to1, to2, to3):
    def one(j, carry):
        for k, out in enumerate((kept, to1, to2, to3)):
            b = jnp.bitwise_xor(pos[3], k) * 7 + j
            out[j] = (own[b] + got[b].astype(f32)).astype(out.dtype)
        return carry

    lax.fori_loop(0, 7, one, 0)


def fold_kernel(pos, own, got1, got2, got3, kept, to1, to2, to3):
    for k, out in enumerate((kept, to1, to2, to3)):
        at = jnp.bitwise_xor(pos[4], k)
        value = own[at] + got1[at].astype(f32) + got2[at].astype(f32) + got3[at].astype(f32)
        out[...] = value.astype(out.dtype)


FACTOR = 1.0 / math.sqrt(CELLS)
PIECE = 9


def write_half(half, src, one, two, wide, sems):
    def emit(out):
        copies = []
        for p in range(0, 27, PIECE):
            wide[p:p + PIECE] = src[p:p + PIECE].astype(f32) * FACTOR
            at = pl.ds(p, PIECE)
            copies.append(pltpu.make_async_copy(wide.at[at], out.at[at], sems.at[p // PIECE]))
            copies[-1].start()
        for copy in copies:
            copy.wait()

    @pl.when(half == 0)
    def _():
        emit(one)

    @pl.when(half != 0)
    def _():
        emit(two)


def mine_kernel(pos, mine, one, two, wide, sems):
    write_half(pos[2], mine, one, two, wide, sems)


def other_kernel(pos, mine, other, one_in, two_in, one, two, bias_one, bias_two, wide, sems, rows_out, row_sems):
    def biases(src):
        rows_out[...] = src[27, 0:16, :].astype(f32) * FACTOR

    @pl.when(pos[2] == 0)
    def _():
        biases(mine)

    @pl.when(pos[2] != 0)
    def _():
        biases(other)

    copies = [
        pltpu.make_async_copy(rows_out.at[pl.ds(8 * i, 1)], out, row_sems.at[i])
        for i, out in enumerate((bias_one, bias_two))
    ]
    for copy in copies:
        copy.start()
    write_half(1 - pos[2], other, one, two, wide, sems)
    for copy in copies:
        copy.wait()


VMEM = pl.BlockSpec(memory_space=pltpu.VMEM)
HBM = pl.BlockSpec(memory_space=pltpu.HBM)
SMEM = pl.BlockSpec(memory_space=pltpu.SMEM)


def call(kernel, out, inputs, scratch, mib, flops, size, places=None, aliases=None):
    return pl.pallas_call(
        kernel,
        out_shape=tuple(jax.ShapeDtypeStruct(*o) for o in out),
        in_specs=inputs,
        out_specs=places or (VMEM,) * len(out),
        scratch_shapes=scratch,
        input_output_aliases=aliases or {},
        compiler_params=pltpu.CompilerParams(vmem_limit_bytes=mib * 1024 * 1024),
        cost_estimate=pl.CostEstimate(flops=flops, bytes_accessed=size, transcendentals=0),
    )


def local(pos, xin, cot, sides, ends, k1, k2, vectors):
    return call(
        local_kernel,
        [
            ((28, 128, 128), bf16), ((128, 128), f32), ((3, 384, 128), bf16),
            ((2, 384, 1024), bf16), ((2, 1024, 384), bf16),
        ],
        [SMEM] + [VMEM] * 7,
        [
            pltpu.VMEM((464, 128), f32),
            pltpu.VMEM((448, 128), f32),
            pltpu.VMEM((3, 448, 384), bf16),
            pltpu.VMEM((3, 448, 384), bf16),
            pltpu.VMEM((3, 384, 128), bf16),
            pltpu.VMEM((3, 384, 128), f32),
            pltpu.VMEM((3, 384, 128), f32),
        ],
        24, 3 * 10**9, 8 * 10**6,
    )(pos, xin, cot, sides, ends, k1, k2, vectors)


def own_grads(pos, field, cotan, biases):
    return call(
        own_kernel, [((28, 128, 128), f32)], [SMEM, VMEM, VMEM, VMEM], [], 16, 10**9, 3 * 10**6,
    )(pos, field, cotan, biases)[0]


def input_grad(d, xin, cot, k1, vectors):
    return call(
        input_kernel,
        [((3, 10, 23, 128), bf16)],
        [VMEM] * 5,
        [
            pltpu.VMEM((400, 128), f32),
            pltpu.VMEM((3, 384, 384), bf16),
            pltpu.VMEM((3, 320, 128), f32),
        ],
        16, 10**9, 3 * 10**6,
    )(d, xin, cot, k1, vectors)[0]


def combine(pos, own, got):
    return call(
        combine_kernel, [((7, 128, 128), f32)] + [((7, 128, 128), bf16)] * 3, [SMEM, VMEM, VMEM], [],
        16, 10**6, 10**6,
    )(pos, own, got)


def fold(pos, kept, got):
    parts = [v.reshape(4, 224, 128) for v in (kept, *got)]
    return call(
        fold_kernel, [((224, 128), f32)] + [((224, 128), bf16)] * 3, [SMEM] + [VMEM] * 4, [], 8, 10**6, 10**6,
    )(pos, *parts)


GRAD = ((27, 128, 128), f32)


def write_mine(pos, mine):
    return call(
        mine_kernel, [GRAD, GRAD], [SMEM, VMEM],
        [pltpu.VMEM(*GRAD), pltpu.SemaphoreType.DMA((3,))],
        8, 10**8, 10**6, (HBM, HBM),
    )(pos, mine)


def write_other(pos, mine, other, one, two):
    bias = ((1, 128), f32)
    return call(
        other_kernel, [GRAD, GRAD, bias, bias], [SMEM, VMEM, VMEM, HBM, HBM],
        [
            pltpu.VMEM(*GRAD), pltpu.SemaphoreType.DMA((3,)),
            pltpu.VMEM((16, 128), f32), pltpu.SemaphoreType.DMA((2,)),
        ],
        8, 10**6, 10**6, (HBM,) * 4, {3: 0, 4: 1},
    )(pos, mine, other, one, two)


def body(block_input, cotangent, kernel_one, bias_one, kernel_two, scale_one, shift_one, scale_two, shift_two):
    xin, cot = jnp.swapaxes(block_input, 1, 2), jnp.swapaxes(cotangent, 1, 2)
    low = jnp.stack([xin[:, :2], cot[:, :2]])
    high = jnp.stack([xin[:, 8:], cot[:, 8:]])
    left, right = exchange(low, high, "wa", 32)

    def edge(s):
        main = jnp.stack([xin[:, :, s], cot[:, :, s]])
        return jnp.concatenate([left[:, :, :, s], main, right[:, :, :, s]], axis=2)

    above, below = exchange(edge(slice(0, 2)), edge(slice(21, 23)), "ha", 8)
    ha, wa = lax.axis_index("ha"), lax.axis_index("wa")
    y, x, c = ha % 4, wa // 8, wa % 2
    one, three = position(x, y, 1), position(x, y, 3)
    first, second = jnp.where(c == 0, one, three), jnp.where(c == 0, three, one)
    pos = jnp.stack([ha * 23 - 2, wa * 10 - 2, c, first, second]).astype(jnp.int32)
    vectors = jnp.pad(jnp.stack([bias_one, scale_one, shift_one, scale_two, shift_two]), ((0, 3), (0, 0)))
    xin, cot, k1, k2 = (jnp.where(wa < 32, v, jnp.zeros_like(v)) for v in (xin, cot, kernel_one, kernel_two))
    send, biases, d, field, cotan = local(pos, xin, cot, jnp.stack([left, right]), jnp.stack([above, below]), k1, k2, vectors)
    got = shifted(send, "c", 2, 1)
    own = own_grads(pos, field, cotan, biases)
    gin = input_grad(d, xin, cot, k1, vectors)
    grad_one, grad_two, grad_bias_one, grad_bias_two = total(pos, own, got)
    shape = (3, 3, 3, 128, 128)
    return (
        jnp.swapaxes(gin, 1, 2), grad_one.reshape(shape), grad_bias_one[0], grad_two.reshape(shape), grad_bias_two[0],
    )


def solution(mesh):
    split = P(None, "ha", "wa", None)
    return jax.shard_map(
        body,
        mesh=mesh,
        in_specs=(split, split) + (P(),) * 7,
        out_specs=(split,) + (P(),) * 4,
        check_vma=False,
    )
```

```python
import math

import jax
import jax.numpy as jnp
from jax import lax
from jax.experimental import pallas as pl
from jax.experimental.pallas import tpu as pltpu
from jax.sharding import PartitionSpec as P

CELLS = 176640
AXES = ("ha", "wa")
f32 = jnp.float32
bf16 = jnp.bfloat16


def coords(d):
    return {"zl": d // 128, "y": (d // 32) % 4, "x": (d // 8) % 4, "zh": (d // 2) % 4, "c": d % 2}


def device_of(p):
    return (((p["zl"] * 4 + p["y"]) * 4 + p["x"]) * 4 + p["zh"]) * 2 + p["c"]


def shift_pairs(axis, size, k):
    pairs = []
    for d in range(256):
        p = coords(d)
        p[axis] = (p[axis] + k) % size
        pairs.append((d, device_of(p)))
    return pairs


def place(v, flip):
    return (v >> 1) ^ (v & 1) if flip == 1 else v >> 1


def position(x, y, flip):
    return place(x, flip) + 2 * place(y, flip)


def flip_pairs(flips, m):
    pairs = []
    for d in range(256):
        p = coords(d)
        p["x"] ^= flips[p["c"]] * (m & 1)
        p["y"] ^= flips[p["c"]] * (m >> 1)
        pairs.append((d, device_of(p)))
    return pairs


def send_pairs(v, pairs):
    return lax.ppermute(v, AXES, pairs)


def shifted(v, axis, size, k):
    return send_pairs(v, shift_pairs(axis, size, k))


def exchange_squares(sends, flips):
    return [send_pairs(sends[m - 1], flip_pairs(flips, m)) for m in (1, 2, 3)]


def gather(v, flips, here):
    got = exchange_squares([v] * 3, flips)
    out = lax.dynamic_update_index_in_dim(jnp.zeros((4,) + v.shape, v.dtype), v, here, 0)
    for m in (2, 1, 3):
        out = lax.dynamic_update_index_in_dim(out, got[m - 1], here ^ m, 0)
    return out


FIRST, SECOND = (1, 3), (3, 1)


def total(pos, own, got):
    first, second = pos[3], pos[4]
    kept, *sends = combine(pos, own, got)
    kept, *sends = fold(pos, kept, exchange_squares(sends, FIRST))
    got = exchange_squares(sends, SECOND)
    v = kept + got[0].astype(f32) + got[1].astype(f32) + got[2].astype(f32)
    v = v + shifted(v, "zl", 2, 1)
    v = v.astype(bf16)
    got = {k: shifted(v, "zh", 4, k) for k in (1, 2, 3)}
    v = ((v.astype(f32) + got[2].astype(f32)) + (got[1].astype(f32) + got[3].astype(f32))).astype(bf16)
    v = gather(v, SECOND, second)
    v = gather(v, FIRST, first).reshape(28, 128, 128)
    other = shifted(v, "c", 2, 1)
    one, two = write_mine(pos, v)
    return write_other(pos, v, other, one, two)


def exchange(low, high, axis, size, odd):
    def swap(first, sent):
        pairs = [(a, b) for i in range(first, size - 1, 2) for a, b in ((i, i + 1), (i + 1, i))]
        return lax.ppermute(sent, axis, pairs)

    far = swap(1, jnp.where(odd, high, low))
    near = swap(0, jnp.where(odd, low, high))
    return near, far


def adjoint(field, k, kw, acc, n):
    for s in range(3):
        w = jnp.concatenate(
            [jnp.concatenate([k[kt, kh, kw] for kh in range(3)], axis=1) for kt in range(2 - s, 3)], axis=0
        )
        part = lax.dot_general(
            field[s, rows(2 - kw, n), :], w, (((1,), (1,)), ((), ())), preferred_element_type=f32
        )
        for j, kt in enumerate(range(2 - s, 3)):
            acc[s - 2 + kt] += part[:, j * 128:(j + 1) * 128]


def slope(z, s):
    return s * (1.0 + z * (1.0 - s))


def rows(i, n):
    return pl.ds(pl.multiple_of(i * 32, 32), n)


def local_kernel(
    pos, xin, cot, sides, ends, k1, k2, vectors,
    send_out, bias_out, d_out, field, cotan,
    line, x_all, a3, g3, a2, acc, acc2,
):
    row0, col0, core, odd = pos[0], pos[1], pos[2], pos[5]
    bias1, scale1, shift1, scale2, shift2 = (vectors[i:i + 1, :] for i in range(5))
    line[...] = jnp.zeros_like(line)
    x_all[...] = jnp.zeros_like(x_all)
    for half in range(2):
        cotan[half, 960:1024, :] = jnp.zeros((64, 384), bf16)

    def masks(first, n):
        q = lax.broadcasted_iota(jnp.int32, (n, 128), 0)
        col, row = (q >> 5) + first, q & 31
        r, c = row + row0, col + col0
        inside = (r >= 0) & (r < 184) & (c >= 0) & (c < 320)
        return (row >= 2) & (row < 25), inside

    def place(dst, base, which, main, t):
        for w in range(14):
            at = base + w * 32
            if 2 <= w < 12:
                dst[at + 2:at + 25, :] = main[t, w - 2].astype(f32)
            else:
                dst[at + 2:at + 25, :] = sides[core if w >= 12 else 1 - core, which, t, w % 12].astype(f32)
            dst[at:at + 2, :] = ends[1 - odd, which, t, w].astype(f32)
            dst[at + 25:at + 27, :] = ends[odd, which, t, w].astype(f32)

    def own_cells(half, t, first):
        at = pl.ds(pl.multiple_of(t * 320, 64), 320)
        for k, o in enumerate((9, 8, 7)):
            cotan[half, at, k * 128:(k + 1) * 128] = line[o + first:o + first + 320, :].astype(bf16)

    def enter(t, bias):
        own, inside = masks(0, 448)
        line[8:456, :] = jnp.zeros((448, 128), f32)
        place(line, 8, 1, cot, t)
        place(x_all, 0, 0, xin, t)
        for k, o in enumerate((9, 8, 7)):
            g3[t, :, k * 128:(k + 1) * 128] = line[o:o + 448, :].astype(bf16)
        go = jnp.where(own, line[8:456, :], 0.0)
        line[8:456, :] = go
        own_cells(1, t, 64)
        z = x_all[...] * scale1 + shift1
        line[8:456, :] = jnp.where(inside, z * jax.nn.sigmoid(z), 0.0)
        for k, o in enumerate((7, 8, 9)):
            a3[t, :, k * 128:(k + 1) * 128] = line[o:o + 448, :].astype(bf16)
        return bias + jnp.sum(go[64:384].reshape(40, 8, 128), axis=0)

    bias_two = lax.fori_loop(0, 3, enter, jnp.zeros((8, 128), f32))
    for t in range(3):
        acc[t] = jnp.zeros((384, 128), f32)
        acc2[t] = jnp.zeros((384, 128), f32)

    def first_convs(kw, carry):
        for s in range(3):
            w = jnp.concatenate(
                [jnp.concatenate([k1[kt, kh, kw] for kh in range(3)], axis=0) for kt in range(s, 3)], axis=1
            )
            part = jnp.dot(a3[s, rows(kw, 384), :], w, preferred_element_type=f32)
            for j, kt in enumerate(range(s, 3)):
                acc[s + 2 - kt] += part[:, j * 128:(j + 1) * 128]
        adjoint(g3, k2, kw, acc2, 384)
        return carry

    lax.fori_loop(0, 3, first_convs, 0)
    line[392:400, :] = jnp.zeros((8, 128), f32)

    def middle(t, bias):
        own, inside = masks(1, 384)
        z = (acc[t] + bias1) * scale2 + shift2
        s = jax.nn.sigmoid(z)
        a2[t] = jnp.where(inside, z * s, 0.0).astype(bf16)
        d = jnp.where(inside, acc2[t] * slope(z, s) * scale2, 0.0).astype(bf16)
        d_out[t] = d
        do = jnp.where(own, d.astype(f32), 0.0)
        line[8:392, :] = do
        own_cells(0, t, 32)
        return bias + jnp.sum(do[32:352].reshape(40, 8, 128), axis=0)

    bias_one = lax.fori_loop(0, 3, middle, jnp.zeros((8, 128), f32))
    tail = [jnp.zeros((64, 128), bf16)]
    for kw in range(3):
        at = slice(kw * 128, (kw + 1) * 128)
        first = [a3[t, (1 + kw) * 32:(1 + kw) * 32 + 320, 128:256] for t in range(3)]
        field[0, at, :] = jnp.transpose(jnp.concatenate(first + tail, axis=0))
        second = [a2[t, kw * 32:kw * 32 + 320, :] for t in range(3)]
        field[1, at, :] = jnp.transpose(jnp.concatenate(second + tail, axis=0))
    low = lax.broadcasted_iota(jnp.int32, (128, 128), 0)
    b1 = jnp.broadcast_to(jnp.sum(bias_one, axis=0, keepdims=True), (128, 128))
    b2 = jnp.broadcast_to(jnp.sum(bias_two, axis=0, keepdims=True), (128, 128))
    biases = jnp.where(low < 8, b1, jnp.where(low < 16, b2, 0.0))
    bias_out[...] = biases
    kernel_grads(field, cotan, 1 - core, biases, send_out)


def kernel_grads(field, cotan, half, biases, out):
    for kt, n in enumerate((384, 640, 1024)):
        start = (2 - kt) * 320
        part = jnp.dot(
            field[half, :, 0:n], cotan[half, start:start + n, :], preferred_element_type=f32
        ).astype(out.dtype)
        for kh in range(3):
            for kw in range(3):
                out[kt * 9 + kh * 3 + kw] = part[kw * 128:(kw + 1) * 128, kh * 128:(kh + 1) * 128]
    out[27] = jnp.where(half == 0, biases, 0.0).astype(out.dtype)


def own_kernel(pos, field, cotan, biases, out):
    kernel_grads(field, cotan, pos[2], biases[...], out)


def input_kernel(d, xin, cot, k1, vectors, gin, line, d3, acc):
    scale1, shift1 = vectors[1:2, :], vectors[2:3, :]
    line[...] = jnp.zeros_like(line)
    for t in range(3):
        acc[t] = jnp.zeros((320, 128), f32)
        line[8:392, :] = d[t].astype(f32)
        for k, o in enumerate((9, 8, 7)):
            d3[t, :, k * 128:(k + 1) * 128] = line[o:o + 384, :].astype(bf16)

    def convs(kw, carry):
        adjoint(d3, k1, kw, acc, 320)
        return carry

    lax.fori_loop(0, 3, convs, 0)
    for t in range(3):
        for w in range(10):
            z = xin[t, w].astype(f32) * scale1 + shift1
            change = acc[t, w * 32 + 2:w * 32 + 25, :] * (slope(z, jax.nn.sigmoid(z)) * scale1)
            gin[t, w] = (cot[t, w].astype(f32) + change).astype(bf16)


def combine_kernel(pos, own, got, kept, to1, to2, to3):
    def one(j, carry):
        for k, out in enumerate((kept, to1, to2, to3)):
            b = jnp.bitwise_xor(pos[3], k) * 7 + j
            out[j] = (own[b] + got[b].astype(f32)).astype(out.dtype)
        return carry

    lax.fori_loop(0, 7, one, 0)


def fold_kernel(pos, own, got1, got2, got3, kept, to1, to2, to3):
    for k, out in enumerate((kept, to1, to2, to3)):
        at = jnp.bitwise_xor(pos[4], k)
        value = own[at] + got1[at].astype(f32) + got2[at].astype(f32) + got3[at].astype(f32)
        out[...] = value.astype(out.dtype)


FACTOR = 1.0 / math.sqrt(CELLS)
PIECE = 9


def write_half(half, src, one, two, wide, sems):
    def emit(out):
        copies = []
        for p in range(0, 27, PIECE):
            wide[p:p + PIECE] = src[p:p + PIECE].astype(f32) * FACTOR
            at = pl.ds(p, PIECE)
            copies.append(pltpu.make_async_copy(wide.at[at], out.at[at], sems.at[p // PIECE]))
            copies[-1].start()
        for copy in copies:
            copy.wait()

    @pl.when(half == 0)
    def _():
        emit(one)

    @pl.when(half != 0)
    def _():
        emit(two)


def mine_kernel(pos, mine, one, two, wide, sems):
    write_half(pos[2], mine, one, two, wide, sems)


def other_kernel(pos, mine, other, one_in, two_in, one, two, bias_one, bias_two, wide, sems, rows_out, row_sems):
    def biases(src):
        rows_out[...] = src[27, 0:16, :].astype(f32) * FACTOR

    @pl.when(pos[2] == 0)
    def _():
        biases(mine)

    @pl.when(pos[2] != 0)
    def _():
        biases(other)

    copies = [
        pltpu.make_async_copy(rows_out.at[pl.ds(8 * i, 1)], out, row_sems.at[i])
        for i, out in enumerate((bias_one, bias_two))
    ]
    for copy in copies:
        copy.start()
    write_half(1 - pos[2], other, one, two, wide, sems)
    for copy in copies:
        copy.wait()


VMEM = pl.BlockSpec(memory_space=pltpu.VMEM)
HBM = pl.BlockSpec(memory_space=pltpu.HBM)
SMEM = pl.BlockSpec(memory_space=pltpu.SMEM)


def call(kernel, out, inputs, scratch, mib, flops, size, places=None, aliases=None):
    return pl.pallas_call(
        kernel,
        out_shape=tuple(jax.ShapeDtypeStruct(*o) for o in out),
        in_specs=inputs,
        out_specs=places or (VMEM,) * len(out),
        scratch_shapes=scratch,
        input_output_aliases=aliases or {},
        compiler_params=pltpu.CompilerParams(vmem_limit_bytes=mib * 1024 * 1024),
        cost_estimate=pl.CostEstimate(flops=flops, bytes_accessed=size, transcendentals=0),
    )


def local(pos, xin, cot, sides, ends, k1, k2, vectors):
    return call(
        local_kernel,
        [
            ((28, 128, 128), bf16), ((128, 128), f32), ((3, 384, 128), bf16),
            ((2, 384, 1024), bf16), ((2, 1024, 384), bf16),
        ],
        [SMEM] + [VMEM] * 7,
        [
            pltpu.VMEM((464, 128), f32),
            pltpu.VMEM((448, 128), f32),
            pltpu.VMEM((3, 448, 384), bf16),
            pltpu.VMEM((3, 448, 384), bf16),
            pltpu.VMEM((3, 384, 128), bf16),
            pltpu.VMEM((3, 384, 128), f32),
            pltpu.VMEM((3, 384, 128), f32),
        ],
        24, 3 * 10**9, 8 * 10**6,
    )(pos, xin, cot, sides, ends, k1, k2, vectors)


def own_grads(pos, field, cotan, biases):
    return call(
        own_kernel, [((28, 128, 128), f32)], [SMEM, VMEM, VMEM, VMEM], [], 16, 10**9, 3 * 10**6,
    )(pos, field, cotan, biases)[0]


def input_grad(d, xin, cot, k1, vectors):
    return call(
        input_kernel,
        [((3, 10, 23, 128), bf16)],
        [VMEM] * 5,
        [
            pltpu.VMEM((400, 128), f32),
            pltpu.VMEM((3, 384, 384), bf16),
            pltpu.VMEM((3, 320, 128), f32),
        ],
        16, 10**9, 3 * 10**6,
    )(d, xin, cot, k1, vectors)[0]


def combine(pos, own, got):
    return call(
        combine_kernel, [((7, 128, 128), f32)] + [((7, 128, 128), bf16)] * 3, [SMEM, VMEM, VMEM], [],
        16, 10**6, 10**6,
    )(pos, own, got)


def fold(pos, kept, got):
    parts = [v.reshape(4, 224, 128) for v in (kept, *got)]
    return call(
        fold_kernel, [((224, 128), f32)] + [((224, 128), bf16)] * 3, [SMEM] + [VMEM] * 4, [], 8, 10**6, 10**6,
    )(pos, *parts)


GRAD = ((27, 128, 128), f32)


def write_mine(pos, mine):
    return call(
        mine_kernel, [GRAD, GRAD], [SMEM, VMEM],
        [pltpu.VMEM(*GRAD), pltpu.SemaphoreType.DMA((3,))],
        8, 10**8, 10**6, (HBM, HBM),
    )(pos, mine)


def write_other(pos, mine, other, one, two):
    bias = ((1, 128), f32)
    return call(
        other_kernel, [GRAD, GRAD, bias, bias], [SMEM, VMEM, VMEM, HBM, HBM],
        [
            pltpu.VMEM(*GRAD), pltpu.SemaphoreType.DMA((3,)),
            pltpu.VMEM((16, 128), f32), pltpu.SemaphoreType.DMA((2,)),
        ],
        8, 10**6, 10**6, (HBM,) * 4, {3: 0, 4: 1},
    )(pos, mine, other, one, two)


def body(block_input, cotangent, kernel_one, bias_one, kernel_two, scale_one, shift_one, scale_two, shift_two):
    xin, cot = jnp.swapaxes(block_input, 1, 2), jnp.swapaxes(cotangent, 1, 2)
    low = jnp.stack([xin[:, :2], cot[:, :2]])
    high = jnp.stack([xin[:, 8:], cot[:, 8:]])
    ha, wa = lax.axis_index("ha"), lax.axis_index("wa")
    y, x, c = ha % 4, wa // 8, wa % 2
    near, far = exchange(low, high, "wa", 32, c == 1)
    left, right = jnp.where(c == 0, far, near), jnp.where(c == 0, near, far)

    def fetch(*arrays):
        return lax.optimization_barrier(tuple(jnp.where(wa < 32, v, jnp.zeros_like(v)) for v in arrays))

    xin, cot = fetch(xin, cot)
    k1, k2 = fetch(kernel_one, kernel_two)
    vectors = jnp.pad(jnp.stack([bias_one, scale_one, shift_one, scale_two, shift_two]), ((0, 3), (0, 0)))

    def edge(s):
        main = jnp.stack([xin[:, :, s], cot[:, :, s]])
        return jnp.concatenate([left[:, :, :, s], main, right[:, :, :, s]], axis=2)

    ends = jnp.stack(exchange(edge(slice(0, 2)), edge(slice(21, 23)), "ha", 8, ha % 2 == 1))
    one, three = position(x, y, 1), position(x, y, 3)
    first, second = jnp.where(c == 0, one, three), jnp.where(c == 0, three, one)
    pos = jnp.stack([ha * 23 - 2, wa * 10 - 2, c, first, second, ha % 2]).astype(jnp.int32)
    send, biases, d, field, cotan = local(pos, xin, cot, jnp.stack([near, far]), ends, k1, k2, vectors)
    got = shifted(send, "c", 2, 1)
    own = own_grads(pos, field, cotan, biases)
    gin = input_grad(d, xin, cot, k1, vectors)
    grad_one, grad_two, grad_bias_one, grad_bias_two = total(pos, own, got)
    shape = (3, 3, 3, 128, 128)
    return (
        jnp.swapaxes(gin, 1, 2), grad_one.reshape(shape), grad_bias_one[0], grad_two.reshape(shape), grad_bias_two[0],
    )


def solution(mesh):
    split = P(None, "ha", "wa", None)
    return jax.shard_map(
        body,
        mesh=mesh,
        in_specs=(split, split) + (P(),) * 7,
        out_specs=(split,) + (P(),) * 4,
        check_vma=False,
    )
```

```python
import math

import jax
import jax.numpy as jnp
from jax import lax
from jax.experimental import pallas as pl
from jax.experimental.pallas import tpu as pltpu
from jax.sharding import PartitionSpec as P

CELLS = 176640
AXES = ("ha", "wa")
f32 = jnp.float32
bf16 = jnp.bfloat16


def coords(d):
    return {"zl": d // 128, "y": (d // 32) % 4, "x": (d // 8) % 4, "zh": (d // 2) % 4, "c": d % 2}


def device_of(p):
    return (((p["zl"] * 4 + p["y"]) * 4 + p["x"]) * 4 + p["zh"]) * 2 + p["c"]


def shift_pairs(axis, size, k):
    pairs = []
    for d in range(256):
        p = coords(d)
        p[axis] = (p[axis] + k) % size
        pairs.append((d, device_of(p)))
    return pairs


def place(v, flip):
    return (v >> 1) ^ (v & 1) if flip == 1 else v >> 1


def position(x, y, flip):
    return place(x, flip) + 2 * place(y, flip)


def flip_pairs(flips, m):
    pairs = []
    for d in range(256):
        p = coords(d)
        p["x"] ^= flips[p["c"]] * (m & 1)
        p["y"] ^= flips[p["c"]] * (m >> 1)
        pairs.append((d, device_of(p)))
    return pairs


def send_pairs(v, pairs):
    return lax.ppermute(v, AXES, pairs)


def shifted(v, axis, size, k):
    return send_pairs(v, shift_pairs(axis, size, k))


def exchange_squares(sends, flips):
    return [send_pairs(sends[m - 1], flip_pairs(flips, m)) for m in (1, 2, 3)]


def gather(v, flips, here):
    got = exchange_squares([v] * 3, flips)
    out = lax.dynamic_update_index_in_dim(jnp.zeros((4,) + v.shape, v.dtype), v, here, 0)
    for m in (2, 1, 3):
        out = lax.dynamic_update_index_in_dim(out, got[m - 1], here ^ m, 0)
    return out


FIRST, SECOND = (1, 3), (3, 1)


def total(pos, own, got):
    first, second = pos[3], pos[4]
    kept, *sends = combine(pos, own, got)
    kept, *sends = fold(pos, kept, exchange_squares(sends, FIRST))
    got = exchange_squares(sends, SECOND)
    v = kept + got[0].astype(f32) + got[1].astype(f32) + got[2].astype(f32)
    v = v.astype(bf16)
    v = (v.astype(f32) + shifted(v, "zl", 2, 1).astype(f32)).astype(bf16)
    got = {k: shifted(v, "zh", 4, k) for k in (1, 2, 3)}
    v = ((v.astype(f32) + got[2].astype(f32)) + (got[1].astype(f32) + got[3].astype(f32))).astype(bf16)
    v = gather(v, SECOND, second)
    v = gather(v, FIRST, first).reshape(28, 128, 128)
    other = shifted(v, "c", 2, 1)
    one, two = write_mine(pos, v)
    return write_other(pos, v, other, one, two)


def exchange(low, high, axis, size, odd):
    def swap(first, sent):
        pairs = [(a, b) for i in range(first, size - 1, 2) for a, b in ((i, i + 1), (i + 1, i))]
        return lax.ppermute(sent, axis, pairs)

    far = swap(1, jnp.where(odd, high, low))
    near = swap(0, jnp.where(odd, low, high))
    return near, far


def adjoint(field, k, kw, acc, n):
    for s in range(3):
        w = jnp.concatenate(
            [jnp.concatenate([k[kt, kh, kw] for kh in range(3)], axis=1) for kt in range(2 - s, 3)], axis=0
        )
        part = lax.dot_general(
            field[s, rows(2 - kw, n), :], w, (((1,), (1,)), ((), ())), preferred_element_type=f32
        )
        for j, kt in enumerate(range(2 - s, 3)):
            acc[s - 2 + kt] += part[:, j * 128:(j + 1) * 128]


def slope(z, s):
    return s * (1.0 + z * (1.0 - s))


def rows(i, n):
    return pl.ds(pl.multiple_of(i * 32, 32), n)


def local_kernel(
    pos, xin, cot, sides, ends, k1, k2, vectors,
    send_out, bias_out, d_out, field, cotan,
    line, x_all, a3, g3, a2, acc, acc2,
):
    row0, col0, core, odd = pos[0], pos[1], pos[2], pos[5]
    bias1, scale1, shift1, scale2, shift2 = (vectors[i:i + 1, :] for i in range(5))
    line[...] = jnp.zeros_like(line)
    x_all[...] = jnp.zeros_like(x_all)
    for half in range(2):
        cotan[half, 960:1024, :] = jnp.zeros((64, 384), bf16)

    def masks(first, n):
        q = lax.broadcasted_iota(jnp.int32, (n, 128), 0)
        col, row = (q >> 5) + first, q & 31
        r, c = row + row0, col + col0
        inside = (r >= 0) & (r < 184) & (c >= 0) & (c < 320)
        return (row >= 2) & (row < 25), inside

    def place(dst, base, which, main, t):
        for w in range(14):
            at = base + w * 32
            if 2 <= w < 12:
                dst[at + 2:at + 25, :] = main[t, w - 2].astype(f32)
            else:
                dst[at + 2:at + 25, :] = sides[core if w >= 12 else 1 - core, which, t, w % 12].astype(f32)
            dst[at:at + 2, :] = ends[1 - odd, which, t, w].astype(f32)
            dst[at + 25:at + 27, :] = ends[odd, which, t, w].astype(f32)

    def own_cells(half, t, first):
        at = pl.ds(pl.multiple_of(t * 320, 64), 320)
        for k, o in enumerate((9, 8, 7)):
            cotan[half, at, k * 128:(k + 1) * 128] = line[o + first:o + first + 320, :].astype(bf16)

    def enter(t, bias):
        own, inside = masks(0, 448)
        line[8:456, :] = jnp.zeros((448, 128), f32)
        place(line, 8, 1, cot, t)
        place(x_all, 0, 0, xin, t)
        for k, o in enumerate((9, 8, 7)):
            g3[t, :, k * 128:(k + 1) * 128] = line[o:o + 448, :].astype(bf16)
        go = jnp.where(own, line[8:456, :], 0.0)
        line[8:456, :] = go
        own_cells(1, t, 64)
        z = x_all[...] * scale1 + shift1
        line[8:456, :] = jnp.where(inside, z * jax.nn.sigmoid(z), 0.0)
        for k, o in enumerate((7, 8, 9)):
            a3[t, :, k * 128:(k + 1) * 128] = line[o:o + 448, :].astype(bf16)
        return bias + jnp.sum(go[64:384].reshape(40, 8, 128), axis=0)

    bias_two = lax.fori_loop(0, 3, enter, jnp.zeros((8, 128), f32))
    for t in range(3):
        acc[t] = jnp.zeros((384, 128), f32)
        acc2[t] = jnp.zeros((384, 128), f32)

    def first_convs(kw, carry):
        for s in range(3):
            w = jnp.concatenate(
                [jnp.concatenate([k1[kt, kh, kw] for kh in range(3)], axis=0) for kt in range(s, 3)], axis=1
            )
            part = jnp.dot(a3[s, rows(kw, 384), :], w, preferred_element_type=f32)
            for j, kt in enumerate(range(s, 3)):
                acc[s + 2 - kt] += part[:, j * 128:(j + 1) * 128]
        adjoint(g3, k2, kw, acc2, 384)
        return carry

    lax.fori_loop(0, 3, first_convs, 0)
    line[392:400, :] = jnp.zeros((8, 128), f32)

    def middle(t, bias):
        own, inside = masks(1, 384)
        z = (acc[t] + bias1) * scale2 + shift2
        s = jax.nn.sigmoid(z)
        a2[t] = jnp.where(inside, z * s, 0.0).astype(bf16)
        d = jnp.where(inside, acc2[t] * slope(z, s) * scale2, 0.0).astype(bf16)
        d_out[t] = d
        do = jnp.where(own, d.astype(f32), 0.0)
        line[8:392, :] = do
        own_cells(0, t, 32)
        return bias + jnp.sum(do[32:352].reshape(40, 8, 128), axis=0)

    bias_one = lax.fori_loop(0, 3, middle, jnp.zeros((8, 128), f32))
    tail = [jnp.zeros((64, 128), bf16)]
    for kw in range(3):
        at = slice(kw * 128, (kw + 1) * 128)
        first = [a3[t, (1 + kw) * 32:(1 + kw) * 32 + 320, 128:256] for t in range(3)]
        field[0, at, :] = jnp.transpose(jnp.concatenate(first + tail, axis=0))
        second = [a2[t, kw * 32:kw * 32 + 320, :] for t in range(3)]
        field[1, at, :] = jnp.transpose(jnp.concatenate(second + tail, axis=0))
    low = lax.broadcasted_iota(jnp.int32, (128, 128), 0)
    b1 = jnp.broadcast_to(jnp.sum(bias_one, axis=0, keepdims=True), (128, 128))
    b2 = jnp.broadcast_to(jnp.sum(bias_two, axis=0, keepdims=True), (128, 128))
    biases = jnp.where(low < 8, b1, jnp.where(low < 16, b2, 0.0))
    bias_out[...] = biases
    kernel_grads(field, cotan, 1 - core, biases, send_out)


def kernel_grads(field, cotan, half, biases, out):
    for kt, n in enumerate((384, 640, 1024)):
        start = (2 - kt) * 320
        part = jnp.dot(
            field[half, :, 0:n], cotan[half, start:start + n, :], preferred_element_type=f32
        ).astype(out.dtype)
        for kh in range(3):
            for kw in range(3):
                out[kt * 9 + kh * 3 + kw] = part[kw * 128:(kw + 1) * 128, kh * 128:(kh + 1) * 128]
    out[27] = jnp.where(half == 0, biases, 0.0).astype(out.dtype)


def own_kernel(pos, field, cotan, biases, out):
    kernel_grads(field, cotan, pos[2], biases[...], out)


def input_kernel(d, xin, cot, k1, vectors, gin, line, d3, acc):
    scale1, shift1 = vectors[1:2, :], vectors[2:3, :]
    line[...] = jnp.zeros_like(line)
    for t in range(3):
        acc[t] = jnp.zeros((320, 128), f32)
        line[8:392, :] = d[t].astype(f32)
        for k, o in enumerate((9, 8, 7)):
            d3[t, :, k * 128:(k + 1) * 128] = line[o:o + 384, :].astype(bf16)

    def convs(kw, carry):
        adjoint(d3, k1, kw, acc, 320)
        return carry

    lax.fori_loop(0, 3, convs, 0)
    for t in range(3):
        for w in range(10):
            z = xin[t, w].astype(f32) * scale1 + shift1
            change = acc[t, w * 32 + 2:w * 32 + 25, :] * (slope(z, jax.nn.sigmoid(z)) * scale1)
            gin[t, w] = (cot[t, w].astype(f32) + change).astype(bf16)


def combine_kernel(pos, own, got, kept, to1, to2, to3):
    def one(j, carry):
        for k, out in enumerate((kept, to1, to2, to3)):
            b = jnp.bitwise_xor(pos[3], k) * 7 + j
            out[j] = (own[b] + got[b].astype(f32)).astype(out.dtype)
        return carry

    lax.fori_loop(0, 7, one, 0)


def fold_kernel(pos, own, got1, got2, got3, kept, to1, to2, to3):
    for k, out in enumerate((kept, to1, to2, to3)):
        at = jnp.bitwise_xor(pos[4], k)
        value = own[at] + got1[at].astype(f32) + got2[at].astype(f32) + got3[at].astype(f32)
        out[...] = value.astype(out.dtype)


FACTOR = 1.0 / math.sqrt(CELLS)
PIECE = 9


def write_half(half, src, one, two, wide, sems):
    def emit(out):
        copies = []
        for p in range(0, 27, PIECE):
            wide[p:p + PIECE] = src[p:p + PIECE].astype(f32) * FACTOR
            at = pl.ds(p, PIECE)
            copies.append(pltpu.make_async_copy(wide.at[at], out.at[at], sems.at[p // PIECE]))
            copies[-1].start()
        for copy in copies:
            copy.wait()

    @pl.when(half == 0)
    def _():
        emit(one)

    @pl.when(half != 0)
    def _():
        emit(two)


def mine_kernel(pos, mine, one, two, wide, sems):
    write_half(pos[2], mine, one, two, wide, sems)


def other_kernel(pos, mine, other, one_in, two_in, one, two, bias_one, bias_two, wide, sems, rows_out, row_sems):
    def biases(src):
        rows_out[...] = src[27, 0:16, :].astype(f32) * FACTOR

    @pl.when(pos[2] == 0)
    def _():
        biases(mine)

    @pl.when(pos[2] != 0)
    def _():
        biases(other)

    copies = [
        pltpu.make_async_copy(rows_out.at[pl.ds(8 * i, 1)], out, row_sems.at[i])
        for i, out in enumerate((bias_one, bias_two))
    ]
    for copy in copies:
        copy.start()
    write_half(1 - pos[2], other, one, two, wide, sems)
    for copy in copies:
        copy.wait()


VMEM = pl.BlockSpec(memory_space=pltpu.VMEM)
HBM = pl.BlockSpec(memory_space=pltpu.HBM)
SMEM = pl.BlockSpec(memory_space=pltpu.SMEM)


def call(kernel, out, inputs, scratch, mib, flops, size, places=None, aliases=None):
    return pl.pallas_call(
        kernel,
        out_shape=tuple(jax.ShapeDtypeStruct(*o) for o in out),
        in_specs=inputs,
        out_specs=places or (VMEM,) * len(out),
        scratch_shapes=scratch,
        input_output_aliases=aliases or {},
        compiler_params=pltpu.CompilerParams(vmem_limit_bytes=mib * 1024 * 1024),
        cost_estimate=pl.CostEstimate(flops=flops, bytes_accessed=size, transcendentals=0),
    )


def local(pos, xin, cot, sides, ends, k1, k2, vectors):
    return call(
        local_kernel,
        [
            ((28, 128, 128), bf16), ((128, 128), f32), ((3, 384, 128), bf16),
            ((2, 384, 1024), bf16), ((2, 1024, 384), bf16),
        ],
        [SMEM] + [VMEM] * 7,
        [
            pltpu.VMEM((464, 128), f32),
            pltpu.VMEM((448, 128), f32),
            pltpu.VMEM((3, 448, 384), bf16),
            pltpu.VMEM((3, 448, 384), bf16),
            pltpu.VMEM((3, 384, 128), bf16),
            pltpu.VMEM((3, 384, 128), f32),
            pltpu.VMEM((3, 384, 128), f32),
        ],
        24, 3 * 10**9, 8 * 10**6,
    )(pos, xin, cot, sides, ends, k1, k2, vectors)


def own_grads(pos, field, cotan, biases):
    return call(
        own_kernel, [((28, 128, 128), f32)], [SMEM, VMEM, VMEM, VMEM], [], 16, 10**9, 3 * 10**6,
    )(pos, field, cotan, biases)[0]


def input_grad(d, xin, cot, k1, vectors):
    return call(
        input_kernel,
        [((3, 10, 23, 128), bf16)],
        [VMEM] * 5,
        [
            pltpu.VMEM((400, 128), f32),
            pltpu.VMEM((3, 384, 384), bf16),
            pltpu.VMEM((3, 320, 128), f32),
        ],
        16, 10**9, 3 * 10**6,
    )(d, xin, cot, k1, vectors)[0]


def combine(pos, own, got):
    return call(
        combine_kernel, [((7, 128, 128), f32)] + [((7, 128, 128), bf16)] * 3, [SMEM, VMEM, VMEM], [],
        16, 10**6, 10**6,
    )(pos, own, got)


def fold(pos, kept, got):
    parts = [v.reshape(4, 224, 128) for v in (kept, *got)]
    return call(
        fold_kernel, [((224, 128), f32)] + [((224, 128), bf16)] * 3, [SMEM] + [VMEM] * 4, [], 8, 10**6, 10**6,
    )(pos, *parts)


GRAD = ((27, 128, 128), f32)


def write_mine(pos, mine):
    return call(
        mine_kernel, [GRAD, GRAD], [SMEM, VMEM],
        [pltpu.VMEM(*GRAD), pltpu.SemaphoreType.DMA((3,))],
        8, 10**8, 10**6, (HBM, HBM),
    )(pos, mine)


def write_other(pos, mine, other, one, two):
    bias = ((1, 128), f32)
    return call(
        other_kernel, [GRAD, GRAD, bias, bias], [SMEM, VMEM, VMEM, HBM, HBM],
        [
            pltpu.VMEM(*GRAD), pltpu.SemaphoreType.DMA((3,)),
            pltpu.VMEM((16, 128), f32), pltpu.SemaphoreType.DMA((2,)),
        ],
        8, 10**6, 10**6, (HBM,) * 4, {3: 0, 4: 1},
    )(pos, mine, other, one, two)


def body(block_input, cotangent, kernel_one, bias_one, kernel_two, scale_one, shift_one, scale_two, shift_two):
    xin, cot = jnp.swapaxes(block_input, 1, 2), jnp.swapaxes(cotangent, 1, 2)
    low = jnp.stack([xin[:, :2], cot[:, :2]])
    high = jnp.stack([xin[:, 8:], cot[:, 8:]])
    ha, wa = lax.axis_index("ha"), lax.axis_index("wa")
    y, x, c = ha % 4, wa // 8, wa % 2
    near, far = exchange(low, high, "wa", 32, c == 1)
    left, right = jnp.where(c == 0, far, near), jnp.where(c == 0, near, far)

    def edge(s):
        main = jnp.stack([xin[:, :, s], cot[:, :, s]])
        return jnp.concatenate([left[:, :, :, s], main, right[:, :, :, s]], axis=2)

    ends = jnp.stack(exchange(edge(slice(0, 2)), edge(slice(21, 23)), "ha", 8, ha % 2 == 1))
    one, three = position(x, y, 1), position(x, y, 3)
    first, second = jnp.where(c == 0, one, three), jnp.where(c == 0, three, one)
    pos = jnp.stack([ha * 23 - 2, wa * 10 - 2, c, first, second, ha % 2]).astype(jnp.int32)
    vectors = jnp.pad(jnp.stack([bias_one, scale_one, shift_one, scale_two, shift_two]), ((0, 3), (0, 0)))
    xin, cot, k1, k2 = (jnp.where(wa < 32, v, jnp.zeros_like(v)) for v in (xin, cot, kernel_one, kernel_two))
    send, biases, d, field, cotan = local(pos, xin, cot, jnp.stack([near, far]), ends, k1, k2, vectors)
    got = shifted(send, "c", 2, 1)
    own = own_grads(pos, field, cotan, biases)
    gin = input_grad(d, xin, cot, k1, vectors)
    grad_one, grad_two, grad_bias_one, grad_bias_two = total(pos, own, got)
    shape = (3, 3, 3, 128, 128)
    return (
        jnp.swapaxes(gin, 1, 2), grad_one.reshape(shape), grad_bias_one[0], grad_two.reshape(shape), grad_bias_two[0],
    )


def solution(mesh):
    split = P(None, "ha", "wa", None)
    return jax.shard_map(
        body,
        mesh=mesh,
        in_specs=(split, split) + (P(),) * 7,
        out_specs=(split,) + (P(),) * 4,
        check_vma=False,
    )
```
